8 devices in a mesh: data: 1 (over z), seq: 8 (over y, x, core).
Axes of the slice: x: 2, y: 2, z: 1, core: 2. Of those that a mesh axis runs over, the one named last changes fastest.
Arguments:
- x_tok: bfloat16 [16384, 1280], P(('data', 'seq'))
- dy_tok: bfloat16 [16384, 1280], P(('data', 'seq'))
- ln_gamma: float32 [1280], replicated
- ln_beta: float32 [1280], replicated
- w_qkv: bfloat16 [1280, 3, 16, 80], replicated
- w_out: bfloat16 [1280, 1280], replicated
Outputs:
- output 1: bfloat16 [16384, 1280], P(('data', 'seq'))
- output 2: bfloat16 [16384, 1280], P(('data', 'seq'))
- output 3: float32 [1280, 3, 16, 80], P(('data', 'seq'))
- output 4: float32 [1280, 1280], P(('data', 'seq'))
- output 5: float32 [1280], P('data')
- output 6: float32 [1280], P('data')
All inputs are finite; a program needn't handle non-finite values.
Results may differ from the reference program's by a relative error of at most 0.00435681.
Values are sent between devices in bfloat16 or wider.
A program may use at most 1 GiB of HBM per device.

```python
import jax
import jax.numpy as jnp
from jax import lax

TOKENS_DEV = 2048
SEQ = 8
D = 1280
HEADS = 16
HEAD = D // HEADS
TOKENS = SEQ * TOKENS_DEV
LN_EPS = 1e-5


def setup_inputs(seed: int = 0, part: int = 0) -> dict:
    part_key = jax.random.fold_in(jax.random.key(seed), part)
    keys_part = jax.random.split(part_key, 5)
    keys_shared = jax.random.split(jax.random.key(seed + 1), 4)
    noise = jax.random.normal(keys_part[0], (SEQ, TOKENS_DEV, D), jnp.float32)
    shard_offs = jax.random.normal(keys_part[1], (SEQ, 1, D), jnp.float32)
    base_offs = 0.7 * jax.random.normal(keys_part[2], (1, 1, D), jnp.float32)
    x_tok = (noise + shard_offs + base_offs).reshape(TOKENS, D).astype(jnp.bfloat16)
    grad_mean = 0.5 * jax.random.normal(keys_part[3], (1, D), jnp.float32)
    dy_tok = (jax.random.normal(keys_part[4], (TOKENS, D), jnp.float32) + grad_mean).astype(jnp.bfloat16)
    ln_gamma = 1.0 + 0.3 * jax.random.normal(keys_shared[0], (D,), jnp.float32)
    ln_beta = 0.5 * jax.random.normal(keys_shared[1], (D,), jnp.float32)
    w_qkv = (jax.random.normal(keys_shared[2], (D, 3, HEADS, HEAD), jnp.float32) * D ** -0.5).astype(jnp.bfloat16)
    w_out = (jax.random.normal(keys_shared[3], (D, D), jnp.float32) * D ** -0.5).astype(jnp.bfloat16)
    return {"x_tok": x_tok, "dy_tok": dy_tok, "ln_gamma": ln_gamma, "ln_beta": ln_beta, "w_qkv": w_qkv, "w_out": w_out}


def phi_act(t):
    return jnp.where(t > 0, t + 1.0, jnp.exp(jnp.minimum(t, 0.0)))


def phi_slope(t):
    return jnp.where(t > 0, 1.0, jnp.exp(jnp.minimum(t, 0.0)))


def reference(x_tok, dy_tok, ln_gamma, ln_beta, w_qkv, w_out):
    x_f32 = x_tok.astype(jnp.float32)
    centered = x_f32 - jnp.mean(x_f32, axis=-1, keepdims=True)
    inv_std = lax.rsqrt(jnp.mean(centered * centered, axis=-1, keepdims=True) + LN_EPS)
    x_hat = centered * inv_std
    normed = (x_hat * ln_gamma + ln_beta).astype(jnp.bfloat16)
    w_flat = w_qkv.reshape(D, 3 * D)
    qkv_all = jnp.dot(normed, w_flat, preferred_element_type=jnp.float32).astype(jnp.bfloat16).reshape(TOKENS, 3, HEADS, HEAD)
    q_raw = qkv_all[:, 0].astype(jnp.float32)
    k_raw = qkv_all[:, 1].astype(jnp.float32)
    v_heads = qkv_all[:, 2].astype(jnp.float32)
    feat_q = phi_act(q_raw).astype(jnp.bfloat16).astype(jnp.float32)
    feat_k = phi_act(k_raw).astype(jnp.bfloat16).astype(jnp.float32)
    state_b = jnp.einsum("nhi,nhj->hij", feat_k, v_heads).astype(jnp.bfloat16).astype(jnp.float32)
    norm_b = jnp.sum(feat_k, axis=0).astype(jnp.bfloat16).astype(jnp.float32)
    numerator = jnp.einsum("nhi,hij->nhj", feat_q, state_b)
    denominator = jnp.einsum("nhi,hi->nh", feat_q, norm_b)
    att_f32 = numerator / denominator[:, :, None]
    att_out = att_f32.astype(jnp.bfloat16).reshape(TOKENS, D)
    y_tok = (x_f32 + jnp.dot(att_out, w_out, preferred_element_type=jnp.float32)).astype(jnp.bfloat16)
    dw_out = jnp.dot(att_out.T, dy_tok, preferred_element_type=jnp.float32)
    d_att = jnp.dot(dy_tok, w_out.T, preferred_element_type=jnp.float32).reshape(TOKENS, HEADS, HEAD)
    g_scaled = (d_att / denominator[:, :, None]).astype(jnp.bfloat16).astype(jnp.float32)
    correction = jnp.sum(g_scaled * att_f32, axis=-1)
    d_fq = jnp.einsum("nhj,hij->nhi", g_scaled, state_b) - correction[:, :, None] * norm_b
    d_state_b = jnp.einsum("nhi,nhj->hij", feat_q, g_scaled).astype(jnp.bfloat16).astype(jnp.float32)
    d_norm = -jnp.einsum("nh,nhi->hi", correction, feat_q)
    d_fk = jnp.einsum("nhj,hij->nhi", v_heads, d_state_b) + d_norm
    d_val = jnp.einsum("nhi,hij->nhj", feat_k, d_state_b)
    d_q = (d_fq * phi_slope(q_raw)).astype(jnp.bfloat16)
    d_k = (d_fk * phi_slope(k_raw)).astype(jnp.bfloat16)
    d_qkv = jnp.stack([d_q, d_k, d_val.astype(jnp.bfloat16)], axis=1).reshape(TOKENS, 3 * D)
    dw_qkv = jnp.dot(normed.T, d_qkv, preferred_element_type=jnp.float32).reshape(D, 3, HEADS, HEAD)
    d_normed = jnp.dot(d_qkv, w_flat.T, preferred_element_type=jnp.float32)
    d_gamma = jnp.sum(d_normed * x_hat, axis=0)
    d_beta = jnp.sum(d_normed, axis=0)
    scaled_grad = d_normed * ln_gamma
    d_ln = inv_std * (scaled_grad - jnp.mean(scaled_grad, axis=-1, keepdims=True) - x_hat * jnp.mean(scaled_grad * x_hat, axis=-1, keepdims=True))
    dx_tok = (dy_tok.astype(jnp.float32) + d_ln).astype(jnp.bfloat16)
    return (y_tok, dx_tok, dw_qkv, dw_out, d_gamma, d_beta)
```

```python
import functools

import jax
import jax.numpy as jnp
from jax import lax
from jax.experimental import pallas as pl
from jax.experimental.pallas import tpu as pltpu
from jax.sharding import PartitionSpec as P

LN_EPS = 1e-5
T = 2048
D = 1280
HD = 80
NH = 16
R = 256
NT_ = T // R
C = 256
NJ = D // C
BW = 512
BAND = [min(max(C * j - 128, 0), D - BW) for j in range(NJ)]
PIECE = D // 8
NCH = 4 * NJ
SLOTS = 8
LAG = 4
f32 = jnp.float32
bf16 = jnp.bfloat16


def dot_nn(a, b):
    return lax.dot_general(a, b, (((1,), (0,)), ((), ())), preferred_element_type=f32)


def dot_nt(a, b):
    return lax.dot_general(a, b, (((1,), (1,)), ((), ())), preferred_element_type=f32)


def dot_tn(a, b):
    return lax.dot_general(a, b, (((0,), (0,)), ((), ())), preferred_element_type=f32)


def phi(t):
    return jnp.where(t > 0, t + 1.0, jnp.exp(jnp.minimum(t, 0.0)))


def slope(t):
    return jnp.where(t > 0, 1.0, jnp.exp(jnp.minimum(t, 0.0)))


def head_of(idx):
    return (idx * 6554) >> 19


def normalise(x):
    centered = x - jnp.mean(x, axis=-1, keepdims=True)
    inv = lax.rsqrt(jnp.mean(centered * centered, axis=-1, keepdims=True) + LN_EPS)
    return centered * inv, inv


def block(x, dy, w_t, w_o, gam, bet,
          y, dx, dw, dgb,
          u_s, g_s, o_s, qkv_s, wo_s, bd_s, zb_s, on_s, tile_s,
          f_s, acc_s, ph_s, pl_s, c_s, st_s, part_s, rsr_s, ag_s, gbr_s, gb_s,
          p_s, r1_s, ra_s, rb_s, ra2_s, rb2_s, ost_s,
          xsem, dsem, ysem, wsem, lsem, osem, ar_send, ar_recv, gb_send, gb_recv,
          dd_send, dd_recv, ln_send, ln_recv):
    s = lax.axis_index("seq")
    core = s % 2
    px = (s // 2) % 2
    py = s // 4
    mate = s + 1 - 2 * core
    xnb = s + 2 - 4 * px
    ynb = s + 4 - 8 * py

    def remote(src, dst, ssem, rsem, dev):
        return pltpu.make_async_remote_copy(src_ref=src, dst_ref=dst, send_sem=ssem, recv_sem=rsem,
                                            device_id={"seq": dev}, device_id_type=pl.DeviceIdType.MESH)

    def rows(t):
        return pl.ds(pl.multiple_of(t * R, R), R)

    def cols(j):
        return pl.ds(pl.multiple_of(j * C, C), C)

    def x_in(t):
        return pltpu.make_async_copy(x.at[rows(t), :], tile_s.at[t % 2], xsem.at[t % 2])

    def dy_in(t):
        return pltpu.make_async_copy(dy.at[rows(t), :], tile_s.at[2 + t % 2], dsem.at[t % 2])

    def tile_out(dst, t):
        return pltpu.make_async_copy(tile_s.at[4 + t % 2], dst.at[rows(t), :], ysem.at[t % 2])

    def w_in(n):
        r = pl.multiple_of(((n + NJ) % (3 * NJ)) * C, C)
        return pltpu.make_async_copy(w_t.at[pl.ds(r, C), :], tile_s.at[2 + n % 3], wsem.at[n % 3])

    dy_all = pltpu.make_async_copy(dy, g_s, lsem.at[0])
    wo_all = pltpu.make_async_copy(w_o, wo_s, lsem.at[1])
    wt_lo = pltpu.make_async_copy(w_t.at[pl.ds(0, T), :], o_s, lsem.at[2])
    wt_hi = pltpu.make_async_copy(w_t.at[pl.ds(T, 3 * D - T), :], g_s.at[pl.ds(0, 3 * D - T), :], lsem.at[0])

    x_in(0).start()
    w_in(0).start()
    w_in(1).start()
    dy_all.start()
    wo_all.start()

    barrier = pltpu.get_barrier_semaphore()
    for k in range(1, 8):
        pl.semaphore_signal(barrier, inc=1, device_id={"seq": (s + k) % 8}, device_id_type=pl.DeviceIdType.MESH)
    pl.semaphore_wait(barrier, 7)

    def pack(a):
        for m in range(110):
            r0, c0 = 8 * (m // 10), 128 * (m % 10)
            part_s[a, m // 14, m % 14] = c_s[r0:r0 + 8, c0:c0 + 128]
        for m in range(110, 112):
            part_s[a, m // 14, m % 14] = jnp.zeros((8, 128), f32)

    def ar_copy(a, phase, k):
        tgt = (s + k) % 8
        if phase == 0:
            return remote(part_s.at[a, tgt], rsr_s.at[a, s], ar_send.at[a, 0, k], ar_recv.at[a, 0, k], tgt)
        return remote(ag_s.at[a, s], ag_s.at[a, s], ar_send.at[a, 1, k], ar_recv.at[a, 1, k], tgt)

    def ar_land(a, phase, k):
        src = (s + 8 - k) % 8
        if phase == 0:
            return remote(part_s.at[a, src], rsr_s.at[a, src], ar_send.at[a, 0, k], ar_recv.at[a, 0, k], src)
        return remote(ag_s.at[a, src], ag_s.at[a, src], ar_send.at[a, 1, k], ar_recv.at[a, 1, k], src)

    def ar_start(a):
        pack(a)
        for k in range(1, 8):
            ar_copy(a, 0, k).start()

    def ar_mid(a):
        total = part_s[a, s]
        for k in range(1, 8):
            ar_land(a, 0, k).wait_recv()
            total = total + rsr_s[a, (s + 8 - k) % 8]
        ag_s[a, s] = total
        for k in range(1, 8):
            ar_copy(a, 1, k).start()

    def ar_end(a):
        for k in range(1, 8):
            ar_land(a, 1, k).wait_recv()
        for k in range(1, 8):
            ar_copy(a, 0, k).wait_send()
            ar_copy(a, 1, k).wait_send()
        for m in range(110):
            r0, c0 = 8 * (m // 10), 128 * (m % 10)
            c_s[r0:r0 + 8, c0:c0 + 128] = ag_s[a, m // 14, m % 14]

    def compact(ref, base, j):
        head = head_of(lax.broadcasted_iota(jnp.int32, (HD, C), 1) + C * j)
        out = jnp.zeros((HD, C), f32)
        for h in range(C * j // HD, (C * j + C - 1) // HD + 1):
            r0 = base + HD * h - BAND[j]
            out = jnp.where(head == h, ref[r0:r0 + HD, :], out)
        c_s[0:HD, C * j:C * j + C] = out

    def expand():
        for h in range(NH):
            c0 = HD * h // 128 * 128
            c1 = -(-(HD * h + HD) // 128) * 128
            head = head_of(lax.broadcasted_iota(jnp.int32, (HD, c1 - c0), 1) + c0)
            bd_s[HD * h:HD * h + HD, c0:c1] = jnp.where(head == h, c_s[0:HD, c0:c1], 0.0).astype(bf16)

    def product(i, lhs, rhs):
        p_s[pl.ds(pl.multiple_of((i % 2) * D, D), D), :] = dot_tn(lhs[...], rhs)

    def dd(i, k):
        src = p_s.at[pl.ds(pl.multiple_of((i % 2) * D + (2 * k + 1 - core) * PIECE, 8), PIECE), :]
        return remote(src, r1_s.at[i % SLOTS, k], dd_send.at[i % 2, k], dd_recv.at[i % 2, k], mate)

    def to_mate(i):
        for k in range(4):
            dd(i, k).start()

    def chip_sum(i):
        for k in range(4):
            dd(i, k).wait_recv()
            own = pl.ds(pl.multiple_of((i % 2) * D + (2 * k + core) * PIECE, 8), PIECE)
            r1_s[i % SLOTS, k] = r1_s[i % SLOTS, k] + p_s[own, :]
            dd(i, k).wait_send()

    def link(i, n):
        slot, q = i % SLOTS, i % LAG
        if n < 2:
            return remote(r1_s.at[slot, 2 * n + 1 - px, :, 0:128], ra_s.at[q, n], ln_send.at[q, n], ln_recv.at[q, n], xnb)
        if n < 4:
            return remote(r1_s.at[slot, 2 * (1 - py) + n - 2, :, 128:256], rb_s.at[q, n - 2], ln_send.at[q, n], ln_recv.at[q, n], ynb)
        if n == 4:
            return remote(r1_s.at[slot, 2 * (1 - py) + px, :, 0:128], ra2_s.at[q], ln_send.at[q, n], ln_recv.at[q, n], ynb)
        return remote(r1_s.at[slot, 2 * py + 1 - px, :, 128:256], rb2_s.at[q], ln_send.at[q, n], ln_recv.at[q, n], xnb)

    def first_hop(i):
        for n in (0, 2, 1, 3):
            link(i, n).start()

    def second_hop(i):
        slot, q = i % SLOTS, i % LAG
        for n in range(2):
            link(i, n).wait_recv()
            r1_s[slot, 2 * n + px, :, 0:128] = r1_s[slot, 2 * n + px, :, 0:128] + ra_s[q, n]
        for n in range(2):
            link(i, n + 2).wait_recv()
            r1_s[slot, 2 * py + n, :, 128:256] = r1_s[slot, 2 * py + n, :, 128:256] + rb_s[q, n]
        link(i, 4).start()
        link(i, 5).start()

    def piece_out(i):
        return pltpu.make_async_copy(ost_s.at[i % 2], dw.at[:, cols(i)], osem.at[i % 2])

    def last_sum(i):
        slot, q = i % SLOTS, i % LAG

        @pl.when(i >= 2)
        def _():
            piece_out(i - 2).wait()

        link(i, 4).wait_recv()
        ost_s[i % 2, :, 0:128] = r1_s[slot, 2 * py + px, :, 0:128] + ra2_s[q]
        link(i, 5).wait_recv()
        ost_s[i % 2, :, 128:256] = r1_s[slot, 2 * py + px, :, 128:256] + rb2_s[q]
        for n in range(6):
            link(i, n).wait_send()
        piece_out(i).start()

    def pump(m, lo, hi):
        @pl.when((m - 4 >= lo) & (m - 4 < hi))
        def _():
            last_sum(m - 4)

        @pl.when((m - 2 >= lo) & (m - 2 < hi))
        def _():
            second_hop(m - 2)

        @pl.when((m >= lo) & (m < hi))
        def _():
            first_hop(m)

    bd_s[...] = jnp.zeros((D, D), bf16)
    gamma = gam[...]
    beta = bet[...]

    @pl.loop(0, NT_)
    def _(t):
        x_in(t).wait()

        @pl.when(t + 1 < NT_)
        def _():
            x_in(t + 1).start()

        x_hat, _ = normalise(tile_s[t % 2].astype(f32))
        u_s[rows(t), :] = (x_hat * gamma + beta).astype(bf16)

    for j in range(NJ):
        hr = head_of(lax.broadcasted_iota(jnp.int32, (C, BW), 0) + C * j)
        hc = head_of(lax.broadcasted_iota(jnp.int32, (C, BW), 1) + BAND[j])
        on_s[j] = jnp.where(hr == hc, 1.0, 0.0).astype(bf16)

    def project(n, which, keep):
        w_in(n).wait()

        @pl.when(n + 2 < 3 * NJ)
        def _():
            w_in(n + 2).start()

        j = n % NJ

        @pl.loop(0, T // 512)
        def _(b):
            r = pl.ds(pl.multiple_of(b * 512, 512), 512)
            out = dot_nt(u_s[r, :], tile_s[2 + n % 3]).astype(bf16)
            qkv_s[which, r, cols(j)] = out
            if keep:
                feat = phi(out.astype(f32)).astype(bf16)
                o_s[r, cols(j)] = feat
                part = jnp.sum(feat.astype(f32), axis=0, keepdims=True)
                before = jnp.where(b == 0, 0.0, c_s[HD:HD + 1, cols(j)])
                c_s[HD:HD + 1, cols(j)] = before + part

    c_s[HD:HD + 8, :] = jnp.zeros((8, D), f32)

    @pl.loop(0, NJ)
    def _(n):
        project(n, 1, True)

    @pl.loop(NJ, 2 * NJ)
    def _(n):
        project(n, 2, False)

    for j in range(NJ):
        st_s[...] = dot_tn(o_s[:, BAND[j]:BAND[j] + BW], qkv_s[2, :, C * j:C * j + C])
        compact(st_s, 0, j)
    ar_start(0)

    @pl.loop(2 * NJ, 3 * NJ - 1)
    def _(n):
        project(n, 0, False)

    ar_mid(0)
    project(3 * NJ - 1, 0, False)
    ar_end(0)
    expand()
    for j in range(NJ):
        z = c_s[HD:HD + 1, BAND[j]:BAND[j] + BW]
        zb_s[j] = jnp.where(on_s[j].astype(f32) > 0.5, jnp.broadcast_to(z, (C, BW)), 0.0).astype(bf16)

    def num_den(j):
        f = f_s[:, BAND[j]:BAND[j] + BW]
        return dot_nn(f, bd_s[BAND[j]:BAND[j] + BW, C * j:C * j + C]), dot_nt(f, zb_s[j])

    @pl.loop(0, NT_)
    def _(t):
        f_s[...] = phi(qkv_s[0, rows(t), :].astype(f32)).astype(bf16)
        for j in range(NJ):
            num, den = num_den(j)
            o_s[rows(t), C * j:C * j + C] = (num / den).astype(bf16)

    dy_all.wait()
    wo_all.wait()

    @pl.loop(0, NJ)
    def _(i):
        product(i, o_s, g_s[:, cols(i)])

        @pl.when(i > 0)
        def _():
            chip_sum(i - 1)

        to_mate(i)

        @pl.when(i == 1)
        def _():
            pump(0, 0, NJ)

    chip_sum(NJ - 1)
    pump(1, 0, NJ)

    p_s[...] = jnp.zeros((2 * D, C), f32)
    st_s[0:8, 0:C] = jnp.zeros((8, C), f32)
    gb_s[...] = jnp.zeros((8, D), f32)

    @pl.loop(0, NT_)
    def _(t):
        acc_s[...] = dot_nt(g_s[rows(t), :], wo_s[...])
        f_s[...] = phi(qkv_s[0, rows(t), :].astype(f32)).astype(bf16)
        for j in range(NJ):
            cj = slice(C * j, C * j + C)
            num, den = num_den(j)
            g = (acc_s[:, cj] / den).astype(bf16)
            g_s[rows(t), cj] = g
            prod = g.astype(f32) * (num / den)
            high = prod.astype(bf16)
            ph_s[:, cj] = high
            pl_s[:, cj] = (prod - high.astype(f32)).astype(bf16)
        for j in range(NJ):
            cj = slice(C * j, C * j + C)
            band = slice(BAND[j], BAND[j] + BW)
            corr = dot_nt(ph_s[:, band], on_s[j]) + dot_nt(pl_s[:, band], on_s[j])
            d_f = dot_nt(g_s[rows(t), band], bd_s[cj, band]) - corr * c_s[HD:HD + 1, cj].astype(bf16).astype(f32)
            raw = qkv_s[0, rows(t), cj].astype(f32)
            qkv_s[0, rows(t), cj] = (d_f * slope(raw)).astype(bf16)
            gb_s[0:1, cj] = gb_s[0:1, cj] + jnp.sum(corr * f_s[:, cj].astype(f32), axis=0, keepdims=True)
            p_s[BW * j:BW * j + BW, :] = p_s[BW * j:BW * j + BW, :] + dot_tn(f_s[:, band], g_s[rows(t), cj])

        @pl.when(t % 2 == 1)
        def _():
            pump(2 + t // 2, 0, NJ)

    for j in range(NJ):
        compact(p_s, BW * j, j)
    c_s[HD:HD + 1, :] = -gb_s[0:1, :]
    ar_start(1)
    wt_hi.start()

    @pl.loop(6, 9)
    def _(m):
        pump(m, 0, NJ)

    def weight_chunk(i):
        n = i - NJ
        product(i, u_s, qkv_s[n // NJ, :, cols(n % NJ)])

    @pl.loop(NJ, 2 * NJ)
    def _(i):
        weight_chunk(i)

        @pl.when(i > NJ)
        def _():
            chip_sum(i - 1)

        to_mate(i)

        @pl.when((i == NJ + 1) | (i == NJ + 3))
        def _():
            pump(NJ + (i - NJ) // 2, NJ, NCH)

    chip_sum(2 * NJ - 1)
    ar_mid(1)

    x_in(0).start()

    @pl.loop(0, NT_)
    def _(t):
        x_in(t).wait()

        @pl.when(t + 1 < NT_)
        def _():
            x_in(t + 1).start()

        @pl.when(t >= 2)
        def _():
            tile_out(y, t - 2).wait()

        tile_s[4 + t % 2] = (tile_s[t % 2].astype(f32) + dot_nn(o_s[rows(t), :], wo_s[...])).astype(bf16)
        tile_out(y, t).start()

        @pl.when(t % 4 == 3)
        def _():
            pump(NJ + 2 + t // 4, NJ, NCH)

    wt_lo.start()
    tile_out(y, NT_ - 2).wait()
    tile_out(y, NT_ - 1).wait()
    ar_end(1)
    expand()

    @pl.loop(0, NT_)
    def _(t):
        f_s[...] = phi(qkv_s[1, rows(t), :].astype(f32)).astype(bf16)
        ph_s[...] = qkv_s[2, rows(t), :]
        for j in range(NJ):
            cj = slice(C * j, C * j + C)
            band = slice(BAND[j], BAND[j] + BW)
            d_f = dot_nt(ph_s[:, band], bd_s[cj, band]) + c_s[HD:HD + 1, cj]
            raw = qkv_s[1, rows(t), cj].astype(f32)
            qkv_s[1, rows(t), cj] = (d_f * slope(raw)).astype(bf16)
            qkv_s[2, rows(t), cj] = dot_nn(f_s[:, band], bd_s[band, cj]).astype(bf16)

        @pl.when(t == 3)
        def _():
            pump(NJ + 4, NJ, NCH)

    @pl.loop(2 * NJ, 2 * NJ + 2)
    def _(i):
        weight_chunk(i)

        @pl.when(i > 2 * NJ)
        def _():
            chip_sum(i - 1)

        to_mate(i)

    gb_s[...] = jnp.zeros((8, D), f32)
    x_in(0).start()
    dy_in(0).start()
    wt_lo.wait()
    wt_hi.wait()

    @pl.loop(0, NT_)
    def _(t):
        pump(2 * NJ + t, NJ, NCH)
        weight_chunk(2 * NJ + 2 + t)
        chip_sum(2 * NJ + 1 + t)
        to_mate(2 * NJ + 2 + t)
        x_in(t).wait()
        dy_in(t).wait()

        @pl.when(t + 1 < NT_)
        def _():
            x_in(t + 1).start()
            dy_in(t + 1).start()

        @pl.when(t >= 2)
        def _():
            tile_out(dx, t - 2).wait()

        cut = T - D
        for j in range(NJ):
            cj = slice(C * j, C * j + C)
            acc_s[:, cj] = (dot_nn(qkv_s[0, rows(t), :], o_s[0:D, cj])
                            + dot_nn(qkv_s[1, rows(t), 0:cut], o_s[D:T, cj])
                            + dot_nn(qkv_s[1, rows(t), cut:D], g_s[0:D - cut, cj])
                            + dot_nn(qkv_s[2, rows(t), :], g_s[D - cut:2 * D - cut, cj]))
        du = acc_s[...]
        x_hat, inv = normalise(tile_s[t % 2].astype(f32))
        dux = du * x_hat
        gb_s[0:1, :] = gb_s[0:1, :] + jnp.sum(dux, axis=0, keepdims=True)
        gb_s[1:2, :] = gb_s[1:2, :] + jnp.sum(du, axis=0, keepdims=True)
        e = du * gamma
        m1 = jnp.mean(e, axis=-1, keepdims=True)
        m2 = jnp.mean(e * x_hat, axis=-1, keepdims=True)
        tile_s[4 + t % 2] = (tile_s[2 + t % 2].astype(f32) + inv * (e - m1 - x_hat * m2)).astype(bf16)
        tile_out(dx, t).start()

    def gb_copy(k):
        return remote(gb_s, gbr_s.at[k], gb_send.at[k], gb_recv.at[k], (s + k) % 8)

    for k in range(1, 8):
        gb_copy(k).start()
    pump(NCH - 2, NJ, NCH)
    chip_sum(NCH - 1)

    @pl.loop(NCH - 1, NCH + 4)
    def _(m):
        pump(m, NJ, NCH)

    tile_out(dx, NT_ - 2).wait()
    tile_out(dx, NT_ - 1).wait()
    for k in range(1, 8):
        gb_copy(k).wait_recv()
        gb_copy(k).wait_send()
    gbr_s[0] = gb_s[...]
    total = jnp.zeros((8, D), f32)
    for d in range(8):
        total = total + gbr_s[(s + 8 - d) % 8]
    dgb[...] = total
    piece_out(NCH - 2).wait()
    piece_out(NCH - 1).wait()


def local_block(x_tok, dy_tok, ln_gamma, ln_beta, w_qkv, w_out):
    w_t = jnp.transpose(w_qkv, (1, 2, 3, 0)).reshape(3 * D, D)
    hbm = pl.BlockSpec(memory_space=pl.ANY)
    vmem = pl.BlockSpec(memory_space=pltpu.VMEM)
    dma = pltpu.SemaphoreType.DMA
    scratch = [
        pltpu.VMEM((T, D), bf16),
        pltpu.VMEM((T, D), bf16),
        pltpu.VMEM((T, D), bf16),
        pltpu.VMEM((3, T, D), bf16),
        pltpu.VMEM((D, D), bf16),
        pltpu.VMEM((D, D), bf16),
        pltpu.VMEM((NJ, C, BW), bf16),
        pltpu.VMEM((NJ, C, BW), bf16),
        pltpu.VMEM((6, R, D), bf16),
        pltpu.VMEM((R, D), bf16),
        pltpu.VMEM((R, D), f32),
        pltpu.VMEM((R, D), bf16),
        pltpu.VMEM((R, D), bf16),
        pltpu.VMEM((HD + 8, D), f32),
        pltpu.VMEM((BW, C), f32),
        pltpu.VMEM((2, 8, 14, 8, 128), f32),
        pltpu.VMEM((2, 8, 14, 8, 128), f32),
        pltpu.VMEM((2, 8, 14, 8, 128), f32),
        pltpu.VMEM((8, 8, D), f32),
        pltpu.VMEM((8, D), f32),
        pltpu.VMEM((2 * D, C), f32),
        pltpu.VMEM((SLOTS, 4, PIECE, C), f32),
        pltpu.VMEM((LAG, 2, PIECE, 128), f32),
        pltpu.VMEM((LAG, 2, PIECE, 128), f32),
        pltpu.VMEM((LAG, PIECE, 128), f32),
        pltpu.VMEM((LAG, PIECE, 128), f32),
        pltpu.VMEM((2, PIECE, C), f32),
        dma((2,)), dma((2,)), dma((2,)), dma((3,)), dma((3,)), dma((2,)),
        dma((2, 2, 8)), dma((2, 2, 8)), dma((8,)), dma((8,)),
        dma((2, 4)), dma((2, 4)), dma((LAG, 6)), dma((LAG, 6)),
    ]
    y, dx, dw, dgb = pl.pallas_call(
        block,
        name="block",
        out_shape=(jax.ShapeDtypeStruct((T, D), bf16), jax.ShapeDtypeStruct((T, D), bf16),
                   jax.ShapeDtypeStruct((PIECE, 4 * D), f32), jax.ShapeDtypeStruct((8, D), f32)),
        in_specs=[hbm, hbm, hbm, hbm, vmem, vmem],
        out_specs=(hbm, hbm, hbm, vmem),
        scratch_shapes=scratch,
        compiler_params=pltpu.CompilerParams(collective_id=0, has_side_effects=True, vmem_limit_bytes=67043328),
    )(x_tok, dy_tok, w_t, w_out, ln_gamma.reshape(1, D), ln_beta.reshape(1, D))
    return (y, dx, dw[:, D:].reshape(PIECE, 3, NH, HD), dw[:, :D], dgb[0], dgb[1])


def solution(mesh):
    rows = P(("data", "seq"), None)
    return jax.shard_map(
        local_block, mesh=mesh,
        in_specs=(rows, rows, P(None), P(None), P(None, None, None, None), P(None, None)),
        out_specs=(rows, rows, P(("data", "seq"), None, None, None), rows, P("data"), P("data")),
        check_vma=False)
```

```python
import functools

import jax
import jax.numpy as jnp
from jax import lax
from jax.experimental import pallas as pl
from jax.experimental.pallas import tpu as pltpu
from jax.sharding import PartitionSpec as P

LN_EPS = 1e-5
T = 2048
D = 1280
HD = 80
NH = 16
R = 256
G = 32
NT_ = T // R
C = 256
NJ = D // C
BW = 512
BAND = [min(max(C * j - 128, 0), D - BW) for j in range(NJ)]
PIECE = D // 8
NCH = 4 * NJ
SLOTS = 8
LAG = 4
f32 = jnp.float32
bf16 = jnp.bfloat16


def dot_nn(a, b):
    return lax.dot_general(a, b, (((1,), (0,)), ((), ())), preferred_element_type=f32)


def dot_nt(a, b):
    return lax.dot_general(a, b, (((1,), (1,)), ((), ())), preferred_element_type=f32)


def dot_tn(a, b):
    return lax.dot_general(a, b, (((0,), (0,)), ((), ())), preferred_element_type=f32)


def phi(t):
    return jnp.where(t > 0, t + 1.0, jnp.exp(jnp.minimum(t, 0.0)))


def slope(t):
    return jnp.where(t > 0, 1.0, jnp.exp(jnp.minimum(t, 0.0)))


def head_of(idx):
    return (idx * 6554) >> 19


def normalise(x):
    centered = x - jnp.mean(x, axis=-1, keepdims=True)
    inv = lax.rsqrt(jnp.mean(centered * centered, axis=-1, keepdims=True) + LN_EPS)
    return centered * inv, inv


def block(x, dy, w_t, w_o, gam, bet,
          y, dx, dwq, dwo, dgam, dbet,
          u_s, g_s, o_s, qkv_s, wo_s, bd_s, zb_s, on_s, tile_s,
          f_s, acc_s, den_s, ph_s, pl_s, c_s, part_s, rsr_s, ags_s, agd_s, gbr_s, gb_s,
          p_s, r1_s, ra_s, rb_s, ra2_s, rb2_s, ost_s,
          xsem, dsem, ysem, wsem, lsem, osem, ar_send, ar_recv, gb_send, gb_recv,
          dd_send, dd_recv, ln_send, ln_recv):
    s = lax.axis_index("seq")
    core = s % 2
    px = (s // 2) % 2
    py = s // 4
    mate = s + 1 - 2 * core
    xnb = s + 2 - 4 * px
    ynb = s + 4 - 8 * py

    def remote(src, dst, ssem, rsem, dev):
        return pltpu.make_async_remote_copy(src_ref=src, dst_ref=dst, send_sem=ssem, recv_sem=rsem,
                                            device_id={"seq": dev}, device_id_type=pl.DeviceIdType.MESH)

    def rows(t):
        return pl.ds(pl.multiple_of(t * R, R), R)

    def cols(j):
        return pl.ds(pl.multiple_of(j * C, C), C)

    def x_in(t):
        return pltpu.make_async_copy(x.at[rows(t), :], tile_s.at[t % 2], xsem.at[t % 2])

    def dy_in(t):
        return pltpu.make_async_copy(dy.at[rows(t), :], tile_s.at[2 + t % 2], dsem.at[t % 2])

    def tile_out(dst, t):
        return pltpu.make_async_copy(tile_s.at[4 + t % 2], dst.at[rows(t), :], ysem.at[t % 2])

    def w_in(n):
        r = pl.multiple_of(((n + NJ) % (3 * NJ)) * C, C)
        return pltpu.make_async_copy(w_t.at[pl.ds(r, C), :], tile_s.at[2 + n % 3], wsem.at[n % 3])

    dy_all = pltpu.make_async_copy(dy, g_s, lsem.at[0])
    wo_all = pltpu.make_async_copy(w_o, wo_s, lsem.at[1])
    wt_lo = pltpu.make_async_copy(w_t.at[pl.ds(0, T), :], o_s, lsem.at[2])
    wt_hi = pltpu.make_async_copy(w_t.at[pl.ds(T, 3 * D - T), :], g_s.at[pl.ds(0, 3 * D - T), :], lsem.at[0])

    x_in(0).start()
    w_in(0).start()
    w_in(1).start()

    barrier = pltpu.get_barrier_semaphore()
    for k in range(1, 8):
        pl.semaphore_signal(barrier, inc=1, device_id={"seq": (s + k) % 8}, device_id_type=pl.DeviceIdType.MESH)

    def pack(a):
        for m in range(110):
            r0, c0 = 8 * (m // 10), 128 * (m % 10)
            part_s[m // 14, m % 14] = c_s[r0:r0 + 8, c0:c0 + 128]
        for m in range(110, 112):
            part_s[m // 14, m % 14] = jnp.zeros((8, 128), f32)

    def ag(a):
        return agd_s if a else ags_s

    def ar_copy(a, phase, k):
        tgt = (s + k) % 8
        if phase == 0:
            return remote(part_s.at[tgt], rsr_s.at[s], ar_send.at[a, 0, k], ar_recv.at[a, 0, k], tgt)
        return remote(ag(a).at[s], ag(a).at[s], ar_send.at[a, 1, k], ar_recv.at[a, 1, k], tgt)

    def ar_land(a, phase, k):
        src = (s + 8 - k) % 8
        if phase == 0:
            return remote(part_s.at[src], rsr_s.at[src], ar_send.at[a, 0, k], ar_recv.at[a, 0, k], src)
        return remote(ag(a).at[src], ag(a).at[src], ar_send.at[a, 1, k], ar_recv.at[a, 1, k], src)

    def ar_start(a):
        pack(a)
        for k in range(1, 8):
            ar_copy(a, 0, k).start()

    def ar_mid(a):
        total = part_s[s]
        for k in range(1, 8):
            ar_land(a, 0, k).wait_recv()
            total = total + rsr_s[(s + 8 - k) % 8]
        ag(a)[s] = total.astype(ag(a).dtype)
        for k in range(1, 8):
            ar_copy(a, 1, k).start()

    def ar_end(a):
        for k in range(1, 8):
            ar_land(a, 1, k).wait_recv()
        for k in range(1, 8):
            ar_copy(a, 0, k).wait_send()
            ar_copy(a, 1, k).wait_send()
        for m in range(110):
            r0, c0 = 8 * (m // 10), 128 * (m % 10)
            c_s[r0:r0 + 8, c0:c0 + 128] = ag(a)[m // 14, m % 14].astype(f32)

    def compact(ref, base, j):
        head = head_of(lax.broadcasted_iota(jnp.int32, (HD, C), 1) + C * j)
        out = jnp.zeros((HD, C), f32)
        for h in range(C * j // HD, (C * j + C - 1) // HD + 1):
            r0 = base + HD * h - BAND[j]
            out = jnp.where(head == h, ref[r0:r0 + HD, :], out)
        c_s[0:HD, C * j:C * j + C] = out

    def expand():
        for h in range(NH):
            c0 = HD * h // 128 * 128
            c1 = -(-(HD * h + HD) // 128) * 128
            head = head_of(lax.broadcasted_iota(jnp.int32, (HD, c1 - c0), 1) + c0)
            bd_s[HD * h:HD * h + HD, c0:c1] = jnp.where(head == h, c_s[0:HD, c0:c1], 0.0).astype(bf16)

    def product(i, lhs, rhs):
        p_s[pl.ds(pl.multiple_of((i % 2) * D, D), D), :] = dot_tn(lhs[...], rhs)

    def dd(i, k):
        src = p_s.at[pl.ds(pl.multiple_of((i % 2) * D + (2 * k + 1 - core) * PIECE, 8), PIECE), :]
        return remote(src, r1_s.at[i % SLOTS, k], dd_send.at[i % 2, k], dd_recv.at[i % 2, k], mate)

    def to_mate(i):
        for k in range(4):
            dd(i, k).start()

    def chip_sum(i):
        for k in range(4):
            dd(i, k).wait_recv()
            own = pl.ds(pl.multiple_of((i % 2) * D + (2 * k + core) * PIECE, 8), PIECE)
            r1_s[i % SLOTS, k] = r1_s[i % SLOTS, k] + p_s[own, :]
            dd(i, k).wait_send()

    def link(i, n):
        slot, q = i % SLOTS, i % LAG
        if n < 2:
            return remote(r1_s.at[slot, 2 * n + 1 - px, :, 0:128], ra_s.at[q, n], ln_send.at[q, n], ln_recv.at[q, n], xnb)
        if n < 4:
            return remote(r1_s.at[slot, 2 * (1 - py) + n - 2, :, 128:256], rb_s.at[q, n - 2], ln_send.at[q, n], ln_recv.at[q, n], ynb)
        if n == 4:
            return remote(r1_s.at[slot, 2 * (1 - py) + px, :, 0:128], ra2_s.at[q], ln_send.at[q, n], ln_recv.at[q, n], ynb)
        return remote(r1_s.at[slot, 2 * py + 1 - px, :, 128:256], rb2_s.at[q], ln_send.at[q, n], ln_recv.at[q, n], xnb)

    def first_hop(i):
        for n in (0, 2, 1, 3):
            link(i, n).start()

    def second_hop(i):
        slot, q = i % SLOTS, i % LAG
        for n in range(2):
            link(i, n).wait_recv()
            r1_s[slot, 2 * n + px, :, 0:128] = r1_s[slot, 2 * n + px, :, 0:128] + ra_s[q, n]
        for n in range(2):
            link(i, n + 2).wait_recv()
            r1_s[slot, 2 * py + n, :, 128:256] = r1_s[slot, 2 * py + n, :, 128:256] + rb_s[q, n]
        link(i, 4).start()
        link(i, 5).start()

    def piece_out(i, first=False):
        dst = dwo.at[:, cols(i)] if first else dwq.at[:, cols(i - NJ)]
        return pltpu.make_async_copy(ost_s.at[i % 2], dst, osem.at[i % 2])

    def last_sum(i):
        slot, q = i % SLOTS, i % LAG

        @pl.when(i >= 2)
        def _():
            pltpu.make_async_copy(ost_s.at[i % 2], dwq.at[:, 0:C], osem.at[i % 2]).wait()

        link(i, 4).wait_recv()
        ost_s[i % 2, :, 0:128] = r1_s[slot, 2 * py + px, :, 0:128] + ra2_s[q]
        link(i, 5).wait_recv()
        ost_s[i % 2, :, 128:256] = r1_s[slot, 2 * py + px, :, 128:256] + rb2_s[q]
        for n in range(6):
            link(i, n).wait_send()

        @pl.when(i < NJ)
        def _():
            piece_out(i, True).start()

        @pl.when(i >= NJ)
        def _():
            piece_out(i).start()

    def pump(m, lo, hi):
        @pl.when((m - 4 >= lo) & (m - 4 < hi))
        def _():
            last_sum(m - 4)

        @pl.when((m - 2 >= lo) & (m - 2 < hi))
        def _():
            second_hop(m - 2)

        @pl.when((m >= lo) & (m < hi))
        def _():
            first_hop(m)

    gamma = gam[...].reshape(1, D)
    beta = bet[...].reshape(1, D)

    @pl.loop(0, NT_)
    def _(t):
        x_in(t).wait()

        @pl.when(t + 1 < NT_)
        def _():
            x_in(t + 1).start()

        for g in range(R // G):
            x_hat, _ = normalise(tile_s[t % 2, G * g:G * g + G, :].astype(f32))
            u_s[pl.ds(pl.multiple_of(t * R + G * g, G), G), :] = (x_hat * gamma + beta).astype(bf16)

    dy_all.start()
    wo_all.start()

    def project(n, which, keep):
        w_in(n).wait()

        @pl.when(n + 2 < 3 * NJ)
        def _():
            w_in(n + 2).start()

        j = n % NJ
        out = dot_nt(u_s[...], tile_s[2 + n % 3]).astype(bf16)
        qkv_s[which, :, cols(j)] = out
        if keep:
            feat = phi(out.astype(f32)).astype(bf16)
            o_s[:, cols(j)] = feat
            c_s[HD:HD + 1, cols(j)] = jnp.sum(feat.astype(f32), axis=0, keepdims=True)

    c_s[HD:HD + 8, :] = jnp.zeros((8, D), f32)

    @pl.loop(0, NJ)
    def _(n):
        project(n, 1, True)

    @pl.loop(NJ, 2 * NJ)
    def _(n):
        project(n, 2, False)

    for j in range(NJ):
        p_s[BW * j:BW * j + BW, :] = dot_tn(o_s[:, BAND[j]:BAND[j] + BW], qkv_s[2, :, C * j:C * j + C])
        compact(p_s, BW * j, j)
    pl.semaphore_wait(barrier, 7)
    ar_start(0)

    @pl.loop(2 * NJ, 3 * NJ - 2)
    def _(n):
        project(n, 0, False)

    ar_mid(0)
    @pl.loop(3 * NJ - 2, 3 * NJ)
    def _(n):
        project(n, 0, False)

    bd_s[...] = jnp.zeros((D, D), bf16)
    for j in range(NJ):
        hr = head_of(lax.broadcasted_iota(jnp.int32, (C, BW), 0) + C * j)
        hc = head_of(lax.broadcasted_iota(jnp.int32, (C, BW), 1) + BAND[j])
        on_s[j] = jnp.where(hr == hc, 1.0, 0.0).astype(bf16)

    ar_end(0)
    expand()
    for j in range(NJ):
        z = c_s[HD:HD + 1, BAND[j]:BAND[j] + BW]
        zb_s[j] = jnp.where(on_s[j].astype(f32) > 0.5, jnp.broadcast_to(z, (C, BW)), 0.0).astype(bf16)

    def num_den(j):
        f = f_s[:, BAND[j]:BAND[j] + BW]
        return dot_nn(f, bd_s[BAND[j]:BAND[j] + BW, C * j:C * j + C]), dot_nt(f, zb_s[j])

    @pl.loop(0, NT_)
    def _(t):
        f_s[...] = phi(qkv_s[0, rows(t), :].astype(f32)).astype(bf16)
        for j in range(NJ):
            num, den = num_den(j)
            o_s[rows(t), C * j:C * j + C] = (num / den).astype(bf16)

    dy_all.wait()
    wo_all.wait()

    @pl.loop(0, NJ)
    def _(i):
        product(i, o_s, g_s[:, cols(i)])

        @pl.when(i > 0)
        def _():
            chip_sum(i - 1)

        to_mate(i)

        @pl.when((i == 1) | (i == 3))
        def _():
            first_hop((i - 1) // 2)

    chip_sum(NJ - 1)
    second_hop(0)
    first_hop(2)

    p_s[...] = jnp.zeros((2 * D, C), f32)
    gb_s[...] = jnp.zeros((2, 8, D), f32)

    @pl.loop(0, NT_)
    def _(t):
        acc_s[...] = dot_nt(g_s[rows(t), :], wo_s[...])
        f_s[...] = phi(qkv_s[0, rows(t), :].astype(f32)).astype(bf16)
        for j in range(NJ):
            cj = slice(C * j, C * j + C)
            den = dot_nt(f_s[:, BAND[j]:BAND[j] + BW], zb_s[j])
            den_s[:, cj] = den
            g_s[rows(t), cj] = (acc_s[:, cj] / den).astype(bf16)
        for j in range(NJ):
            cj = slice(C * j, C * j + C)
            band = slice(BAND[j], BAND[j] + BW)
            back = dot_nt(g_s[rows(t), band], bd_s[cj, band])
            acc_s[:, cj] = back
            prod = f_s[:, cj].astype(f32) / den_s[:, cj] * back
            high = prod.astype(bf16)
            ph_s[:, cj] = high
            pl_s[:, cj] = (prod - high.astype(f32)).astype(bf16)
        for j in range(NJ):
            cj = slice(C * j, C * j + C)
            band = slice(BAND[j], BAND[j] + BW)
            corr = dot_nt(ph_s[:, band], on_s[j]) + dot_nt(pl_s[:, band], on_s[j])
            d_f = acc_s[:, cj] - corr * c_s[HD:HD + 1, cj].astype(bf16).astype(f32)
            raw = qkv_s[0, rows(t), cj].astype(f32)
            qkv_s[0, rows(t), cj] = (d_f * slope(raw)).astype(bf16)
            gb_s[0, 0:1, cj] = gb_s[0, 0:1, cj] + jnp.sum(corr * f_s[:, cj].astype(f32), axis=0, keepdims=True)
            p_s[BW * j:BW * j + BW, :] = p_s[BW * j:BW * j + BW, :] + dot_tn(f_s[:, band], g_s[rows(t), cj])

        @pl.when(t % 2 == 1)
        def _():
            pump(3 + t // 2, 0, NJ)

    for j in range(NJ):
        compact(p_s, BW * j, j)
    c_s[HD:HD + 1, :] = -gb_s[0, 0:1, :]
    ar_start(1)
    wt_hi.start()

    def weight_chunk(i):
        n = i - NJ
        product(i, u_s, qkv_s[n // NJ, :, cols(n % NJ)])

    @pl.loop(NJ, 2 * NJ)
    def _(i):
        weight_chunk(i)

        @pl.when(i > NJ)
        def _():
            chip_sum(i - 1)

        to_mate(i)

        @pl.when((i == NJ + 1) | (i == NJ + 3))
        def _():
            first_hop(NJ + (i - NJ) // 2)

        @pl.when(i < NJ + 2)
        def _():
            last_sum(i - 2)

        @pl.when(i == NJ + 2)
        def _():
            ar_mid(1)

    chip_sum(2 * NJ - 1)

    ar_end(1)
    expand()

    @pl.loop(0, NT_)
    def _(t):
        f_s[...] = phi(qkv_s[1, rows(t), :].astype(f32)).astype(bf16)
        ph_s[...] = qkv_s[2, rows(t), :]
        for j in range(NJ):
            cj = slice(C * j, C * j + C)
            band = slice(BAND[j], BAND[j] + BW)
            d_f = dot_nt(ph_s[:, band], bd_s[cj, band]) + c_s[HD:HD + 1, cj]
            raw = qkv_s[1, rows(t), cj].astype(f32)
            qkv_s[1, rows(t), cj] = (d_f * slope(raw)).astype(bf16)
            qkv_s[2, rows(t), cj] = dot_nn(f_s[:, band], bd_s[band, cj]).astype(bf16)

        @pl.when(t % 3 == 1)
        def _():
            pump(NJ + 2 + t // 3, NJ, NCH)

    x_in(0).start()
    weight_chunk(2 * NJ)
    to_mate(2 * NJ)

    @pl.loop(0, NT_)
    def _(t):
        @pl.when(t % 2 == 0)
        def _():
            i = 2 * NJ + 1 + t // 2
            weight_chunk(i)
            chip_sum(i - 1)
            to_mate(i)
            pump(i - 1, NJ, NCH)

        x_in(t).wait()

        @pl.when(t + 1 < NT_)
        def _():
            x_in(t + 1).start()

        @pl.when(t >= 2)
        def _():
            tile_out(y, t - 2).wait()

        tile_s[4 + t % 2] = (tile_s[t % 2].astype(f32) + dot_nn(o_s[rows(t), :], wo_s[...])).astype(bf16)
        tile_out(y, t).start()

    wt_lo.start()
    tile_out(y, NT_ - 2).wait()
    tile_out(y, NT_ - 1).wait()

    gb_s[...] = jnp.zeros((2, 8, D), f32)
    x_in(0).start()
    dy_in(0).start()

    @pl.loop(0, NT_)
    def _(t):
        @pl.when(t < NJ)
        def _():
            weight_chunk(3 * NJ + t)

        @pl.when(t <= NJ)
        def _():
            chip_sum(3 * NJ - 1 + t)

        @pl.when(t < NJ)
        def _():
            to_mate(3 * NJ + t)

        pump(3 * NJ - 1 + t, NJ, NCH)

        @pl.when(t == 0)
        def _():
            wt_lo.wait()
            wt_hi.wait()

        x_in(t).wait()
        dy_in(t).wait()

        @pl.when(t + 1 < NT_)
        def _():
            x_in(t + 1).start()
            dy_in(t + 1).start()

        @pl.when(t >= 2)
        def _():
            tile_out(dx, t - 2).wait()

        cut = T - D

        @pl.loop(0, NJ)
        def _(j):
            cj = cols(j)
            acc_s[:, cj] = (dot_nn(qkv_s[0, rows(t), :], o_s[0:D, cj])
                            + dot_nn(qkv_s[1, rows(t), 0:cut], o_s[D:T, cj])
                            + dot_nn(qkv_s[1, rows(t), cut:D], g_s[0:D - cut, cj])
                            + dot_nn(qkv_s[2, rows(t), :], g_s[D - cut:2 * D - cut, cj]))

        for g in range(R // G):
            gs = slice(G * g, G * g + G)
            x_hat, inv = normalise(tile_s[t % 2, gs, :].astype(f32))
            du = acc_s[gs, :]
            dux = du * x_hat
            gb_s[0] = gb_s[0] + sum(dux[8 * q:8 * q + 8, :] for q in range(G // 8))
            gb_s[1] = gb_s[1] + sum(du[8 * q:8 * q + 8, :] for q in range(G // 8))
            e = du * gamma
            m1 = jnp.mean(e, axis=-1, keepdims=True)
            m2 = jnp.mean(e * x_hat, axis=-1, keepdims=True)
            tile_s[4 + t % 2, gs, :] = (tile_s[2 + t % 2, gs, :].astype(f32) + inv * (e - m1 - x_hat * m2)).astype(bf16)

        tile_out(dx, t).start()

    def gb_copy(k):
        return remote(gbr_s.at[0], gbr_s.at[k], gb_send.at[k], gb_recv.at[k], (s + k) % 8)

    for n in range(2):
        gbr_s[0, n:n + 1, :] = jnp.sum(gb_s[n], axis=0, keepdims=True)
    for k in range(1, 8):
        gb_copy(k).start()

    @pl.loop(NCH + 2, NCH + 4)
    def _(m):
        pump(m, NJ, NCH)

    tile_out(dx, NT_ - 2).wait()
    tile_out(dx, NT_ - 1).wait()
    for k in range(1, 8):
        gb_copy(k).wait_recv()
        gb_copy(k).wait_send()
    total = jnp.zeros((2, D), f32)
    for d in range(8):
        total = total + gbr_s[(s + 8 - d) % 8]
    dgam[...] = total[0]
    dbet[...] = total[1]
    piece_out(NCH - 2).wait()
    piece_out(NCH - 1).wait()


def local_block(x_tok, dy_tok, ln_gamma, ln_beta, w_qkv, w_out):
    w_t = jnp.transpose(w_qkv, (1, 2, 3, 0)).reshape(3 * D, D)
    hbm = pl.BlockSpec(memory_space=pl.ANY)
    vmem = pl.BlockSpec(memory_space=pltpu.VMEM)
    dma = pltpu.SemaphoreType.DMA
    scratch = [
        pltpu.VMEM((T, D), bf16),
        pltpu.VMEM((T, D), bf16),
        pltpu.VMEM((T, D), bf16),
        pltpu.VMEM((3, T, D), bf16),
        pltpu.VMEM((D, D), bf16),
        pltpu.VMEM((D, D), bf16),
        pltpu.VMEM((NJ, C, BW), bf16),
        pltpu.VMEM((NJ, C, BW), bf16),
        pltpu.VMEM((6, R, D), bf16),
        pltpu.VMEM((R, D), bf16),
        pltpu.VMEM((R, D), f32),
        pltpu.VMEM((R, D), f32),
        pltpu.VMEM((R, D), bf16),
        pltpu.VMEM((R, D), bf16),
        pltpu.VMEM((HD + 8, D), f32),
        pltpu.VMEM((8, 14, 8, 128), f32),
        pltpu.VMEM((8, 14, 8, 128), f32),
        pltpu.VMEM((8, 14, 8, 128), bf16),
        pltpu.VMEM((8, 14, 8, 128), f32),
        pltpu.VMEM((8, 2, D), f32),
        pltpu.VMEM((2, 8, D), f32),
        pltpu.VMEM((2 * D, C), f32),
        pltpu.VMEM((SLOTS, 4, PIECE, C), f32),
        pltpu.VMEM((LAG, 2, PIECE, 128), f32),
        pltpu.VMEM((LAG, 2, PIECE, 128), f32),
        pltpu.VMEM((LAG, PIECE, 128), f32),
        pltpu.VMEM((LAG, PIECE, 128), f32),
        pltpu.VMEM((2, PIECE, C), f32),
        dma((2,)), dma((2,)), dma((2,)), dma((3,)), dma((3,)), dma((2,)),
        dma((2, 2, 8)), dma((2, 2, 8)), dma((8,)), dma((8,)),
        dma((2, 4)), dma((2, 4)), dma((LAG, 6)), dma((LAG, 6)),
    ]
    y, dx, dwq, dwo, dgam, dbet = pl.pallas_call(
        block,
        name="block",
        out_shape=(jax.ShapeDtypeStruct((T, D), bf16), jax.ShapeDtypeStruct((T, D), bf16),
                   jax.ShapeDtypeStruct((PIECE, 3 * D), f32), jax.ShapeDtypeStruct((PIECE, D), f32),
                   jax.ShapeDtypeStruct((D,), f32), jax.ShapeDtypeStruct((D,), f32)),
        in_specs=[hbm, hbm, hbm, hbm, vmem, vmem],
        out_specs=(hbm, hbm, hbm, hbm, vmem, vmem),
        scratch_shapes=scratch,
        compiler_params=pltpu.CompilerParams(collective_id=0, has_side_effects=True, vmem_limit_bytes=67043328),
    )(x_tok, dy_tok, w_t, w_out, ln_gamma, ln_beta)
    return (y, dx, dwq.reshape(PIECE, 3, NH, HD), dwo, dgam, dbet)


def solution(mesh):
    rows = P(("data", "seq"), None)
    return jax.shard_map(
        local_block, mesh=mesh,
        in_specs=(rows, rows, P(None), P(None), P(None, None, None, None), P(None, None)),
        out_specs=(rows, rows, P(("data", "seq"), None, None, None), rows, P("data"), P("data")),
        check_vma=False)
```

```python
import functools

import jax
import jax.numpy as jnp
from jax import lax
from jax.experimental import pallas as pl
from jax.experimental.pallas import tpu as pltpu
from jax.sharding import PartitionSpec as P

LN_EPS = 1e-5
T = 2048
D = 1280
HD = 80
NH = 16
R = 256
G = 32
NT_ = T // R
C = 256
NJ = D // C
BW = 512
BAND = [min(max(C * j - 128, 0), D - BW) for j in range(NJ)]
PIECE = D // 8
NCH = 4 * NJ
SLOTS = 8
LAG = 4
f32 = jnp.float32
bf16 = jnp.bfloat16


def dot_nn(a, b):
    return lax.dot_general(a, b, (((1,), (0,)), ((), ())), preferred_element_type=f32)


def dot_nt(a, b):
    return lax.dot_general(a, b, (((1,), (1,)), ((), ())), preferred_element_type=f32)


def dot_tn(a, b):
    return lax.dot_general(a, b, (((0,), (0,)), ((), ())), preferred_element_type=f32)


def phi(t):
    return jnp.where(t > 0, t + 1.0, jnp.exp(jnp.minimum(t, 0.0)))


def slope(t):
    return jnp.where(t > 0, 1.0, jnp.exp(jnp.minimum(t, 0.0)))


def head_of(idx):
    return (idx * 6554) >> 19


def normalise(x):
    centered = x - jnp.mean(x, axis=-1, keepdims=True)
    inv = lax.rsqrt(jnp.mean(centered * centered, axis=-1, keepdims=True) + LN_EPS)
    return centered * inv, inv


def block(x, dy, w_t, w_o, gam, bet,
          y, dx, dwq, dwo, dgam, dbet,
          u_s, g_s, o_s, qkv_s, wo_s, bd_s, zb_s, on_s, tile_s,
          f_s, acc_s, den_s, ph_s, pl_s, c_s, zz_s, part_s, rsr_s, ag_s, gbr_s, gb_s,
          p_s, r1_s, ra_s, rb_s, ra2_s, rb2_s, ost_s,
          fsem, xsem, dsem, ysem, wsem, lsem, osem, z_send, z_recv, ar_send, ar_recv, gb_send, gb_recv,
          dd_send, dd_recv, ln_send, ln_recv):
    s = lax.axis_index("seq")
    core = s % 2
    px = (s // 2) % 2
    py = s // 4
    mate = s + 1 - 2 * core
    xnb = s + 2 - 4 * px
    ynb = s + 4 - 8 * py

    def remote(src, dst, ssem, rsem, dev):
        return pltpu.make_async_remote_copy(src_ref=src, dst_ref=dst, send_sem=ssem, recv_sem=rsem,
                                            device_id={"seq": dev}, device_id_type=pl.DeviceIdType.MESH)

    def rows(t):
        return pl.ds(pl.multiple_of(t * R, R), R)

    def cols(j):
        return pl.ds(pl.multiple_of(j * C, C), C)

    def slot(n):
        return pl.ds(pl.multiple_of(n * R, R), R)

    def x_in(t):
        return pltpu.make_async_copy(x.at[rows(t), :], tile_s.at[slot(t % 2), :], xsem.at[t % 2])

    def dy_in(t):
        return pltpu.make_async_copy(dy.at[rows(t), :], tile_s.at[slot(2 + t % 2), :], dsem.at[t % 2])

    def tile_out(dst, t):
        return pltpu.make_async_copy(tile_s.at[slot(4 + t % 2), :], dst.at[rows(t), :], ysem.at[t % 2])

    def w_in(n):
        def ge(k):
            return int(n >= k) if isinstance(n, int) else (n >= k).astype(jnp.int32)

        r = n + 5 + 2 * ge(3) - 4 * ge(5) + 2 * ge(7) - 15 * ge(10)
        return pltpu.make_async_copy(w_t.at[cols(r), :], tile_s.at[slot(2 + n % 3), :], wsem.at[n % 3])

    dy_all = pltpu.make_async_copy(dy, g_s, lsem.at[0])
    wo_all = pltpu.make_async_copy(w_o, wo_s, lsem.at[1])
    wt_lo = pltpu.make_async_copy(w_t.at[pl.ds(0, T), :], o_s, lsem.at[2])
    wt_hi = pltpu.make_async_copy(w_t.at[pl.ds(T, 3 * D - T), :], g_s.at[pl.ds(0, 3 * D - T), :], lsem.at[0])

    def x_first(t):
        return pltpu.make_async_copy(x.at[rows(t), :], qkv_s.at[0, rows(t), :], fsem.at[t])

    for t in range(NT_):
        x_first(t).start()
        if t == 1:
            w_in(0).start()
            w_in(1).start()

    barrier = pltpu.get_barrier_semaphore()
    for k in range(1, 8):
        pl.semaphore_signal(barrier, inc=1, device_id={"seq": (s + k) % 8}, device_id_type=pl.DeviceIdType.MESH)

    tiles = [[(r, c) for r in range(10) for c in cs] for cs in (range(4), range(4, 10), range(10))]
    share = ((0, 5), (5, 13), (0, 13))

    def place(a, m):
        lo, hi = share[a]
        return m // (hi - lo), lo + m % (hi - lo)

    def ar_copy(a, phase, k, landing=False):
        dev = (s + 8 - k) % 8 if landing else (s + k) % 8
        lo, hi = share[a]
        sems = ar_send.at[a, phase, k], ar_recv.at[a, phase, k], dev
        if phase == 0:
            row = dev if landing else s
            return remote(part_s.at[dev, lo:hi], rsr_s.at[row, lo:hi], *sems)
        row = dev if landing else s
        return remote(ag_s.at[row, lo:hi], ag_s.at[row, lo:hi], *sems)

    def z_copy(b, k, landing=False):
        dev = (s + 8 - k) % 8 if landing else (s + k) % 8
        row = dev if landing else s
        return remote(zz_s.at[b, row], zz_s.at[b, row], z_send.at[b, k], z_recv.at[b, k], dev)

    def z_start(b):
        for k in range(1, 8):
            z_copy(b, k).start()

    def z_end(b):
        for k in range(1, 8):
            z_copy(b, k, True).wait_recv()
        for k in range(1, 8):
            z_copy(b, k).wait_send()
        total = zz_s[b, 0]
        for d in range(1, 8):
            total = total + zz_s[b, d]
        c_s[HD:HD + 1, :] = total

    def ar_start(a):
        for m, (r, c) in enumerate(tiles[a]):
            d, p = place(a, m)
            part_s[d, p] = c_s[8 * r:8 * r + 8, 128 * c:128 * c + 128]
        for k in range(1, 8):
            ar_copy(a, 0, k).start()

    def ar_mid(a):
        lo, hi = share[a]
        total = part_s[s, lo:hi]
        for k in range(1, 8):
            ar_copy(a, 0, k, True).wait_recv()
            total = total + rsr_s[(s + 8 - k) % 8, lo:hi]
        ag_s[s, lo:hi] = total.astype(bf16)
        for k in range(1, 8):
            ar_copy(a, 1, k).start()

    def ar_end(a):
        for k in range(1, 8):
            ar_copy(a, 1, k, True).wait_recv()
        for k in range(1, 8):
            ar_copy(a, 0, k).wait_send()
            ar_copy(a, 1, k).wait_send()
        for m, (r, c) in enumerate(tiles[a]):
            d, p = place(a, m)
            c_s[8 * r:8 * r + 8, 128 * c:128 * c + 128] = ag_s[d, p].astype(f32)

    def compact(ref, base, j):
        head = head_of(lax.broadcasted_iota(jnp.int32, (HD, C), 1) + C * j)
        out = jnp.zeros((HD, C), f32)
        for h in range(C * j // HD, (C * j + C - 1) // HD + 1):
            r0 = base + HD * h - BAND[j]
            out = jnp.where(head == h, ref[r0:r0 + HD, :], out)
        c_s[0:HD, C * j:C * j + C] = out

    def expand():
        for h in range(NH):
            c0 = HD * h // 128 * 128
            c1 = -(-(HD * h + HD) // 128) * 128
            head = head_of(lax.broadcasted_iota(jnp.int32, (HD, c1 - c0), 1) + c0)
            bd_s[HD * h:HD * h + HD, c0:c1] = jnp.where(head == h, c_s[0:HD, c0:c1], 0.0).astype(bf16)

    def product(i, lhs, rhs):
        p_s[pl.ds(pl.multiple_of((i % 2) * D, D), D), :] = dot_tn(lhs[...], rhs)

    def dd(i, k):
        src = p_s.at[pl.ds(pl.multiple_of((i % 2) * D + (2 * k + 1 - core) * PIECE, 8), PIECE), :]
        return remote(src, r1_s.at[i % SLOTS, k], dd_send.at[i % 2, k], dd_recv.at[i % 2, k], mate)

    def to_mate(i):
        for k in range(4):
            dd(i, k).start()

    def chip_sum(i):
        for k in range(4):
            dd(i, k).wait_recv()
            own = pl.ds(pl.multiple_of((i % 2) * D + (2 * k + core) * PIECE, 8), PIECE)
            r1_s[i % SLOTS, k] = r1_s[i % SLOTS, k] + p_s[own, :]
            dd(i, k).wait_send()

    def link(i, n):
        sl, q = i % SLOTS, i % LAG
        if n < 2:
            return remote(r1_s.at[sl, 2 * n + 1 - px, :, 0:128], ra_s.at[q, n], ln_send.at[q, n], ln_recv.at[q, n], xnb)
        if n < 4:
            return remote(r1_s.at[sl, 2 * (1 - py) + n - 2, :, 128:256], rb_s.at[q, n - 2], ln_send.at[q, n], ln_recv.at[q, n], ynb)
        if n == 4:
            return remote(r1_s.at[sl, 2 * (1 - py) + px, :, 0:128], ra2_s.at[q], ln_send.at[q, n], ln_recv.at[q, n], ynb)
        return remote(r1_s.at[sl, 2 * py + 1 - px, :, 128:256], rb2_s.at[q], ln_send.at[q, n], ln_recv.at[q, n], xnb)

    def first_hop(i):
        for n in (0, 2, 1, 3):
            link(i, n).start()

    def second_hop(i):
        sl, q = i % SLOTS, i % LAG
        for n in range(2):
            link(i, n).wait_recv()
            r1_s[sl, 2 * n + px, :, 0:128] = r1_s[sl, 2 * n + px, :, 0:128] + ra_s[q, n]
        for n in range(2):
            link(i, n + 2).wait_recv()
            r1_s[sl, 2 * py + n, :, 128:256] = r1_s[sl, 2 * py + n, :, 128:256] + rb_s[q, n]
        link(i, 4).start()
        link(i, 5).start()

    def piece_out(i, first=False):
        dst = dwo.at[:, cols(i)] if first else dwq.at[:, cols(i - NJ)]
        return pltpu.make_async_copy(ost_s.at[i % 2], dst, osem.at[i % 2])

    def last_sum(i):
        sl, q = i % SLOTS, i % LAG

        @pl.when(i >= 2)
        def _():
            pltpu.make_async_copy(ost_s.at[i % 2], dwq.at[:, 0:C], osem.at[i % 2]).wait()

        link(i, 4).wait_recv()
        ost_s[i % 2, :, 0:128] = r1_s[sl, 2 * py + px, :, 0:128] + ra2_s[q]
        link(i, 5).wait_recv()
        ost_s[i % 2, :, 128:256] = r1_s[sl, 2 * py + px, :, 128:256] + rb2_s[q]
        for n in range(6):
            link(i, n).wait_send()

        @pl.when(i < NJ)
        def _():
            piece_out(i, True).start()

        @pl.when(i >= NJ)
        def _():
            piece_out(i).start()

    def pump(m, lo, hi):
        @pl.when((m - 4 >= lo) & (m - 4 < hi))
        def _():
            last_sum(m - 4)

        @pl.when((m - 2 >= lo) & (m - 2 < hi))
        def _():
            second_hop(m - 2)

        @pl.when((m >= lo) & (m < hi))
        def _():
            first_hop(m)

    gamma = gam[...].reshape(1, D)
    beta = bet[...].reshape(1, D)

    @pl.loop(0, NT_)
    def _(t):
        x_first(t).wait()
        for g in range(R // G):
            r = pl.ds(pl.multiple_of(t * R + G * g, G), G)
            x_hat, _ = normalise(qkv_s[0, r, :].astype(f32))
            u_s[r, :] = (x_hat * gamma + beta).astype(bf16)

    dy_all.start()

    def project(n, which, j, keep=False):
        w_in(n).wait()

        @pl.when(n + 2 < 3 * NJ)
        def _():
            w_in(n + 2).start()

        out = dot_nt(u_s[...], tile_s[slot(2 + n % 3), :]).astype(bf16)
        qkv_s[which, :, cols(j)] = out
        if keep:
            feat = phi(out.astype(f32)).astype(bf16)
            o_s[:, cols(j)] = feat
            zz_s[0, s, :, cols(j)] = jnp.sum(feat.astype(f32), axis=0, keepdims=True)

    def state(lo, hi):
        for j in range(lo, hi):
            p_s[BW * j:BW * j + BW, :] = dot_tn(o_s[:, BAND[j]:BAND[j] + BW], qkv_s[2, :, C * j:C * j + C])
            compact(p_s, BW * j, j)

    @pl.loop(0, 3)
    def _(n):
        project(n, 1, n, True)

    @pl.loop(3, 5)
    def _(n):
        project(n, 2, n - 3)

    state(0, 2)
    pl.semaphore_wait(barrier, 7)
    ar_start(0)

    @pl.loop(5, 7)
    def _(n):
        project(n, 1, n - 2, True)

    z_start(0)

    @pl.loop(7, 10)
    def _(n):
        project(n, 2, n - 5)

    ar_mid(0)
    state(2, 5)
    ar_start(1)

    @pl.loop(10, 13)
    def _(n):
        project(n, 0, n - 10)

    ar_mid(1)

    @pl.loop(13, 15)
    def _(n):
        project(n, 0, n - 10)

    wo_all.start()
    bd_s[...] = jnp.zeros((D, D), bf16)
    for j in range(NJ):
        hr = head_of(lax.broadcasted_iota(jnp.int32, (C, BW), 0) + C * j)
        hc = head_of(lax.broadcasted_iota(jnp.int32, (C, BW), 1) + BAND[j])
        on_s[j] = jnp.where(hr == hc, 1.0, 0.0).astype(bf16)

    z_end(0)
    ar_end(0)
    ar_end(1)
    expand()
    for j in range(NJ):
        z = c_s[HD:HD + 1, BAND[j]:BAND[j] + BW]
        zb_s[j] = jnp.where(on_s[j].astype(f32) > 0.5, jnp.broadcast_to(z, (C, BW)), 0.0).astype(bf16)

    def num_den(j):
        f = f_s[:, BAND[j]:BAND[j] + BW]
        return dot_nn(f, bd_s[BAND[j]:BAND[j] + BW, C * j:C * j + C]), dot_nt(f, zb_s[j])

    @pl.loop(0, NT_)
    def _(t):
        f_s[...] = phi(qkv_s[0, rows(t), :].astype(f32)).astype(bf16)
        for j in range(NJ):
            num, den = num_den(j)
            o_s[rows(t), C * j:C * j + C] = (num / den).astype(bf16)

    def y_tile(t):
        x_in(t).wait()

        @pl.when(t + 1 < NT_)
        def _():
            x_in(t + 1).start()

        @pl.when(t >= 2)
        def _():
            tile_out(y, t - 2).wait()

        sum_ = tile_s[slot(t % 2), :].astype(f32) + dot_nn(o_s[rows(t), :], wo_s[...])
        tile_s[slot(4 + t % 2), :] = sum_.astype(bf16)
        tile_out(y, t).start()

    x_in(0).start()
    dy_all.wait()
    wo_all.wait()

    @pl.loop(0, NJ)
    def _(i):
        product(i, o_s, g_s[:, cols(i)])

        @pl.when(i > 0)
        def _():
            chip_sum(i - 1)

        to_mate(i)

        @pl.when((i == 1) | (i == 3))
        def _():
            first_hop((i - 1) // 2)

    y_tile(0)
    chip_sum(NJ - 1)
    second_hop(0)
    first_hop(2)

    p_s[...] = jnp.zeros((2 * D, C), f32)
    gb_s[...] = jnp.zeros((2, 8, D), f32)

    @pl.loop(0, NT_)
    def _(t):
        acc_s[...] = dot_nt(g_s[rows(t), :], wo_s[...])
        f_s[...] = phi(qkv_s[0, rows(t), :].astype(f32)).astype(bf16)
        for j in range(NJ):
            cj = slice(C * j, C * j + C)
            den = dot_nt(f_s[:, BAND[j]:BAND[j] + BW], zb_s[j])
            den_s[:, cj] = den
            g_s[rows(t), cj] = (acc_s[:, cj] / den).astype(bf16)
        for j in range(NJ):
            cj = slice(C * j, C * j + C)
            band = slice(BAND[j], BAND[j] + BW)
            back = dot_nt(g_s[rows(t), band], bd_s[cj, band])
            acc_s[:, cj] = back
            prod = f_s[:, cj].astype(f32) / den_s[:, cj] * back
            high = prod.astype(bf16)
            ph_s[:, cj] = high
            pl_s[:, cj] = (prod - high.astype(f32)).astype(bf16)
        for j in range(NJ):
            cj = slice(C * j, C * j + C)
            band = slice(BAND[j], BAND[j] + BW)
            corr = dot_nt(ph_s[:, band], on_s[j]) + dot_nt(pl_s[:, band], on_s[j])
            d_f = acc_s[:, cj] - corr * c_s[HD:HD + 1, cj].astype(bf16).astype(f32)
            raw = qkv_s[0, rows(t), cj].astype(f32)
            qkv_s[0, rows(t), cj] = (d_f * slope(raw)).astype(bf16)
            gb_s[0, 0:1, cj] = gb_s[0, 0:1, cj] + jnp.sum(corr * f_s[:, cj].astype(f32), axis=0, keepdims=True)
            p_s[BW * j:BW * j + BW, :] = p_s[BW * j:BW * j + BW, :] + dot_tn(f_s[:, band], g_s[rows(t), cj])

        @pl.when(t % 2 == 1)
        def _():
            pump(3 + t // 2, 0, NJ)

    for j in range(NJ):
        compact(p_s, BW * j, j)
    zz_s[1, s] = -gb_s[0, 0:1, :]
    ar_start(2)
    z_start(1)
    wt_hi.start()

    def weight_chunk(i):
        n = i - NJ
        product(i, u_s, qkv_s[n // NJ, :, cols(n % NJ)])

    @pl.loop(NJ, 2 * NJ)
    def _(i):
        weight_chunk(i)

        @pl.when(i > NJ)
        def _():
            chip_sum(i - 1)

        to_mate(i)

        @pl.when((i == NJ + 1) | (i == NJ + 3))
        def _():
            first_hop(NJ + (i - NJ) // 2)

        @pl.when(i < NJ + 2)
        def _():
            last_sum(i - 2)

        @pl.when(i == NJ + 2)
        def _():
            ar_mid(2)


    @pl.loop(1, 3)
    def _(t):
        y_tile(t)

    z_end(1)
    ar_end(2)
    chip_sum(2 * NJ - 1)
    pump(NJ + 2, NJ, NCH)
    expand()

    @pl.loop(0, NT_)
    def _(t):
        f_s[...] = phi(qkv_s[1, rows(t), :].astype(f32)).astype(bf16)
        ph_s[...] = qkv_s[2, rows(t), :]
        for j in range(NJ):
            cj = slice(C * j, C * j + C)
            band = slice(BAND[j], BAND[j] + BW)
            d_f = dot_nt(ph_s[:, band], bd_s[cj, band]) + c_s[HD:HD + 1, cj]
            raw = qkv_s[1, rows(t), cj].astype(f32)
            qkv_s[1, rows(t), cj] = (d_f * slope(raw)).astype(bf16)
            qkv_s[2, rows(t), cj] = dot_nn(f_s[:, band], bd_s[band, cj]).astype(bf16)

        @pl.when((t == 3) | (t == 7))
        def _():
            pump(NJ + 3 + t // 7, NJ, NCH)

    @pl.loop(3, NT_)
    def _(t):
        @pl.when(t % 2 == 1)
        def _():
            i = 2 * NJ + (t - 3) // 2
            weight_chunk(i)

            @pl.when(i > 2 * NJ)
            def _():
                chip_sum(i - 1)

            to_mate(i)

            @pl.when(i == 2 * NJ + 1)
            def _():
                pump(2 * NJ, NJ, NCH)

        y_tile(t)

    wt_lo.start()
    tile_out(y, NT_ - 2).wait()
    tile_out(y, NT_ - 1).wait()
    gb_s[...] = jnp.zeros((2, 8, D), f32)
    x_in(0).start()
    dy_in(0).start()

    @pl.loop(0, NT_)
    def _(t):
        @pl.when(t < 7)
        def _():
            weight_chunk(2 * NJ + 3 + t)

        @pl.when(t < 7)
        def _():
            chip_sum(2 * NJ + 2 + t)
            to_mate(2 * NJ + 3 + t)

        @pl.when(t < NT_ - 1)
        def _():
            pump(2 * NJ + 1 + t + t // 4, NJ, NCH)
        @pl.when(t == 0)
        def _():
            wt_lo.wait()
            wt_hi.wait()

        x_in(t).wait()
        dy_in(t).wait()

        @pl.when(t + 1 < NT_)
        def _():
            x_in(t + 1).start()
            dy_in(t + 1).start()

        @pl.when(t >= 2)
        def _():
            tile_out(dx, t - 2).wait()

        cut = T - D

        @pl.loop(0, NJ)
        def _(j):
            cj = cols(j)
            acc_s[:, cj] = (dot_nn(qkv_s[0, rows(t), :], o_s[0:D, cj])
                            + dot_nn(qkv_s[1, rows(t), 0:cut], o_s[D:T, cj])
                            + dot_nn(qkv_s[1, rows(t), cut:D], g_s[0:D - cut, cj])
                            + dot_nn(qkv_s[2, rows(t), :], g_s[D - cut:2 * D - cut, cj]))

        @pl.when(t == 6)
        def _():
            chip_sum(NCH - 1)

        @pl.when((t == 3) | (t >= 6))
        def _():
            pump(2 * NJ + 5 + 4 * (t // 6) + t // 7, NJ, NCH)

        for g in range(R // G):
            gs = slice(G * g, G * g + G)
            x_hat, inv = normalise(tile_s[pl.ds(pl.multiple_of((t % 2) * R + G * g, G), G), :].astype(f32))
            du = acc_s[gs, :]
            dux = du * x_hat
            gb_s[0] = gb_s[0] + sum(dux[8 * q:8 * q + 8, :] for q in range(G // 8))
            gb_s[1] = gb_s[1] + sum(du[8 * q:8 * q + 8, :] for q in range(G // 8))
            e = du * gamma
            m1 = jnp.mean(e, axis=-1, keepdims=True)
            m2 = jnp.mean(e * x_hat, axis=-1, keepdims=True)
            tile_s[pl.ds(pl.multiple_of((4 + t % 2) * R + G * g, G), G), :] = (tile_s[pl.ds(pl.multiple_of((2 + t % 2) * R + G * g, G), G), :].astype(f32) + inv * (e - m1 - x_hat * m2)).astype(bf16)

        tile_out(dx, t).start()

    def gb_copy(k):
        return remote(gbr_s.at[0], gbr_s.at[k], gb_send.at[k], gb_recv.at[k], (s + k) % 8)

    for n in range(2):
        gbr_s[0, n:n + 1, :] = jnp.sum(gb_s[n], axis=0, keepdims=True)
    for k in range(1, 8):
        gb_copy(k).start()

    @pl.loop(NCH + 1, NCH + 4)
    def _(m):
        pump(m, NJ, NCH)

    tile_out(dx, NT_ - 2).wait()
    tile_out(dx, NT_ - 1).wait()
    for k in range(1, 8):
        gb_copy(k).wait_recv()
        gb_copy(k).wait_send()
    total = jnp.zeros((2, D), f32)
    for d in range(8):
        total = total + gbr_s[(s + 8 - d) % 8]
    dgam[...] = total[0]
    dbet[...] = total[1]
    piece_out(NCH - 2).wait()
    piece_out(NCH - 1).wait()


def local_block(x_tok, dy_tok, ln_gamma, ln_beta, w_qkv, w_out):
    w_t = jnp.transpose(w_qkv, (1, 2, 3, 0)).reshape(3 * D, D)
    hbm = pl.BlockSpec(memory_space=pl.ANY)
    vmem = pl.BlockSpec(memory_space=pltpu.VMEM)
    dma = pltpu.SemaphoreType.DMA
    scratch = [
        pltpu.VMEM((T, D), bf16),
        pltpu.VMEM((T, D), bf16),
        pltpu.VMEM((T, D), bf16),
        pltpu.VMEM((3, T, D), bf16),
        pltpu.VMEM((D, D), bf16),
        pltpu.VMEM((D, D), bf16),
        pltpu.VMEM((NJ, C, BW), bf16),
        pltpu.VMEM((NJ, C, BW), bf16),
        pltpu.VMEM((6 * R, D), bf16),
        pltpu.VMEM((R, D), bf16),
        pltpu.VMEM((R, D), f32),
        pltpu.VMEM((R, D), f32),
        pltpu.VMEM((R, D), bf16),
        pltpu.VMEM((R, D), bf16),
        pltpu.VMEM((HD + 8, D), f32),
        pltpu.VMEM((2, 8, 1, D), f32),
        pltpu.VMEM((8, 13, 8, 128), f32),
        pltpu.VMEM((8, 13, 8, 128), f32),
        pltpu.VMEM((8, 13, 8, 128), bf16),
        pltpu.VMEM((8, 2, D), f32),
        pltpu.VMEM((2, 8, D), f32),
        pltpu.VMEM((2 * D, C), f32),
        pltpu.VMEM((SLOTS, 4, PIECE, C), f32),
        pltpu.VMEM((LAG, 2, PIECE, 128), f32),
        pltpu.VMEM((LAG, 2, PIECE, 128), f32),
        pltpu.VMEM((LAG, PIECE, 128), f32),
        pltpu.VMEM((LAG, PIECE, 128), f32),
        pltpu.VMEM((2, PIECE, C), f32),
        dma((NT_,)), dma((2,)), dma((2,)), dma((2,)), dma((3,)), dma((3,)), dma((2,)),
        dma((2, 8)), dma((2, 8)), dma((3, 2, 8)), dma((3, 2, 8)), dma((8,)), dma((8,)),
        dma((2, 4)), dma((2, 4)), dma((LAG, 6)), dma((LAG, 6)),
    ]
    y, dx, dwq, dwo, dgam, dbet = pl.pallas_call(
        block,
        name="block",
        out_shape=(jax.ShapeDtypeStruct((T, D), bf16), jax.ShapeDtypeStruct((T, D), bf16),
                   jax.ShapeDtypeStruct((PIECE, 3 * D), f32), jax.ShapeDtypeStruct((PIECE, D), f32),
                   jax.ShapeDtypeStruct((D,), f32), jax.ShapeDtypeStruct((D,), f32)),
        in_specs=[hbm, hbm, hbm, hbm, vmem, vmem],
        out_specs=(hbm, hbm, hbm, hbm, vmem, vmem),
        scratch_shapes=scratch,
        compiler_params=pltpu.CompilerParams(collective_id=0, has_side_effects=True, vmem_limit_bytes=67043328),
    )(x_tok, dy_tok, w_t, w_out, ln_gamma, ln_beta)
    return (y, dx, dwq.reshape(PIECE, 3, NH, HD), dwo, dgam, dbet)


def solution(mesh):
    rows = P(("data", "seq"), None)
    return jax.shard_map(
        local_block, mesh=mesh,
        in_specs=(rows, rows, P(None), P(None), P(None, None, None, None), P(None, None)),
        out_specs=(rows, rows, P(("data", "seq"), None, None, None), rows, P("data"), P("data")),
        check_vma=False)
```

```python
import functools

import jax
import jax.numpy as jnp
from jax import lax
from jax.experimental import pallas as pl
from jax.experimental.pallas import tpu as pltpu
from jax.sharding import PartitionSpec as P

LN_EPS = 1e-5
T = 2048
D = 1280
HD = 80
NH = 16
R = 256
G = 32
NT_ = T // R
C = 256
NJ = D // C
BW = 512
BAND = [min(max(C * j - 128, 0), D - BW) for j in range(NJ)]
PIECE = D // 8
NCH = 4 * NJ
SLOTS = 8
LAG = 4
f32 = jnp.float32
bf16 = jnp.bfloat16


def dot_nn(a, b):
    return lax.dot_general(a, b, (((1,), (0,)), ((), ())), preferred_element_type=f32)


def dot_nt(a, b):
    return lax.dot_general(a, b, (((1,), (1,)), ((), ())), preferred_element_type=f32)


def dot_tn(a, b):
    return lax.dot_general(a, b, (((0,), (0,)), ((), ())), preferred_element_type=f32)


def phi(t):
    return jnp.where(t > 0, t + 1.0, jnp.exp(jnp.minimum(t, 0.0)))


def slope(t):
    return jnp.where(t > 0, 1.0, jnp.exp(jnp.minimum(t, 0.0)))


def head_of(idx):
    return (idx * 6554) >> 19


def normalise(x):
    centered = x - jnp.mean(x, axis=-1, keepdims=True)
    inv = lax.rsqrt(jnp.mean(centered * centered, axis=-1, keepdims=True) + LN_EPS)
    return centered * inv, inv


def block(x, dy, w_t, w_o, gam, bet,
          y, dx, dwq, dwo, dgam, dbet,
          u_s, g_s, o_s, qkv_s, wo_s, bd_s, zb_s, on_s, tile_s,
          f_s, acc_s, den_s, ph_s, pl_s, c_s, zz_s, part_s, rsr_s, ag_s, gbr_s, gb_s,
          p_s, r1_s, ra_s, rb_s, ra2_s, rb2_s, ost_s,
          fsem, xsem, dsem, ysem, wsem, lsem, osem, z_send, z_recv, ar_send, ar_recv, gb_send, gb_recv,
          dd_send, dd_recv, ln_send, ln_recv):
    s = lax.axis_index("seq")
    core = s % 2
    px = (s // 2) % 2
    py = s // 4
    mate = s + 1 - 2 * core
    xnb = s + 2 - 4 * px
    ynb = s + 4 - 8 * py

    def remote(src, dst, ssem, rsem, dev):
        return pltpu.make_async_remote_copy(src_ref=src, dst_ref=dst, send_sem=ssem, recv_sem=rsem,
                                            device_id={"seq": dev}, device_id_type=pl.DeviceIdType.MESH)

    def rows(t):
        return pl.ds(pl.multiple_of(t * R, R), R)

    def cols(j):
        return pl.ds(pl.multiple_of(j * C, C), C)

    def slot(n):
        return pl.ds(pl.multiple_of(n * R, R), R)

    def x_in(t):
        return pltpu.make_async_copy(x.at[rows(t), :], tile_s.at[slot(t % 2), :], xsem.at[t % 2])

    def dy_in(t):
        return pltpu.make_async_copy(dy.at[rows(t), :], tile_s.at[slot(2 + t % 2), :], dsem.at[t % 2])

    def tile_out(dst, t):
        return pltpu.make_async_copy(tile_s.at[slot(4 + t % 2), :], dst.at[rows(t), :], ysem.at[t % 2])

    def w_in(n):
        def ge(k):
            return int(n >= k) if isinstance(n, int) else (n >= k).astype(jnp.int32)

        r = n + 5 + 2 * ge(3) - 4 * ge(5) + 2 * ge(7) - 15 * ge(10)
        return pltpu.make_async_copy(w_t.at[cols(r), :], tile_s.at[slot(2 + n % 3), :], wsem.at[n % 3])

    dy_all = pltpu.make_async_copy(dy, g_s, lsem.at[0])
    wo_all = pltpu.make_async_copy(w_o, wo_s, lsem.at[1])
    wt_lo = pltpu.make_async_copy(w_t.at[pl.ds(0, T), :], o_s, lsem.at[2])
    wt_hi = pltpu.make_async_copy(w_t.at[pl.ds(T, 3 * D - T), :], g_s.at[pl.ds(0, 3 * D - T), :], lsem.at[0])

    def x_first(t):
        return pltpu.make_async_copy(x.at[rows(t), :], qkv_s.at[0, rows(t), :], fsem.at[t])

    for t in range(NT_):
        x_first(t).start()
        if t == 1:
            w_in(0).start()
            w_in(1).start()

    barrier = pltpu.get_barrier_semaphore()
    for k in range(1, 8):
        pl.semaphore_signal(barrier, inc=1, device_id={"seq": (s + k) % 8}, device_id_type=pl.DeviceIdType.MESH)

    tiles = [[(r, c) for r in range(10) for c in cs] for cs in (range(4), range(4, 10), range(10))]
    share = ((0, 5), (5, 13), (0, 13))

    def place(a, m):
        lo, hi = share[a]
        return m // (hi - lo), lo + m % (hi - lo)

    def ar_copy(a, phase, k, landing=False):
        dev = (s + 8 - k) % 8 if landing else (s + k) % 8
        lo, hi = share[a]
        sems = ar_send.at[a, phase, k], ar_recv.at[a, phase, k], dev
        if phase == 0:
            row = dev if landing else s
            return remote(part_s.at[dev, lo:hi], rsr_s.at[row, lo:hi], *sems)
        row = dev if landing else s
        return remote(ag_s.at[row, lo:hi], ag_s.at[row, lo:hi], *sems)

    def z_copy(b, k, landing=False):
        dev = (s + 8 - k) % 8 if landing else (s + k) % 8
        row = dev if landing else s
        return remote(zz_s.at[b, row], zz_s.at[b, row], z_send.at[b, k], z_recv.at[b, k], dev)

    def z_start(b):
        for k in range(1, 8):
            z_copy(b, k).start()

    def z_end(b):
        for k in range(1, 8):
            z_copy(b, k, True).wait_recv()
        for k in range(1, 8):
            z_copy(b, k).wait_send()
        total = zz_s[b, 0]
        for d in range(1, 8):
            total = total + zz_s[b, d]
        c_s[HD:HD + 1, :] = total

    def ar_start(a):
        for m, (r, c) in enumerate(tiles[a]):
            d, p = place(a, m)
            part_s[d, p] = c_s[8 * r:8 * r + 8, 128 * c:128 * c + 128]
        for k in range(1, 8):
            ar_copy(a, 0, k).start()

    def ar_mid(a):
        lo, hi = share[a]
        total = part_s[s, lo:hi]
        for k in range(1, 8):
            ar_copy(a, 0, k, True).wait_recv()
            total = total + rsr_s[(s + 8 - k) % 8, lo:hi]
        ag_s[s, lo:hi] = total.astype(bf16)
        for k in range(1, 8):
            ar_copy(a, 1, k).start()

    def ar_end(a):
        for k in range(1, 8):
            ar_copy(a, 1, k, True).wait_recv()
        for k in range(1, 8):
            ar_copy(a, 0, k).wait_send()
            ar_copy(a, 1, k).wait_send()
        for m, (r, c) in enumerate(tiles[a]):
            d, p = place(a, m)
            c_s[8 * r:8 * r + 8, 128 * c:128 * c + 128] = ag_s[d, p].astype(f32)

    def compact(ref, base, j):
        head = head_of(lax.broadcasted_iota(jnp.int32, (HD, C), 1) + C * j)
        out = jnp.zeros((HD, C), f32)
        for h in range(C * j // HD, (C * j + C - 1) // HD + 1):
            r0 = base + HD * h - BAND[j]
            out = jnp.where(head == h, ref[r0:r0 + HD, :], out)
        c_s[0:HD, C * j:C * j + C] = out

    def expand():
        for h in range(NH):
            c0 = HD * h // 128 * 128
            c1 = -(-(HD * h + HD) // 128) * 128
            head = head_of(lax.broadcasted_iota(jnp.int32, (HD, c1 - c0), 1) + c0)
            bd_s[HD * h:HD * h + HD, c0:c1] = jnp.where(head == h, c_s[0:HD, c0:c1], 0.0).astype(bf16)

    def product(i, lhs, rhs):
        p_s[pl.ds(pl.multiple_of((i % 2) * D, D), D), :] = dot_tn(lhs[...], rhs)

    def dd(i, k):
        src = p_s.at[pl.ds(pl.multiple_of((i % 2) * D + (2 * k + 1 - core) * PIECE, 8), PIECE), :]
        return remote(src, r1_s.at[i % SLOTS, k], dd_send.at[i % 2, k], dd_recv.at[i % 2, k], mate)

    def to_mate(i):
        for k in range(4):
            dd(i, k).start()

    def chip_sum(i):
        for k in range(4):
            dd(i, k).wait_recv()
            own = pl.ds(pl.multiple_of((i % 2) * D + (2 * k + core) * PIECE, 8), PIECE)
            r1_s[i % SLOTS, k] = r1_s[i % SLOTS, k] + p_s[own, :]
            dd(i, k).wait_send()

    def link(i, n):
        sl, q = i % SLOTS, i % LAG
        if n < 2:
            return remote(r1_s.at[sl, 2 * n + 1 - px, :, 0:128], ra_s.at[q, n], ln_send.at[q, n], ln_recv.at[q, n], xnb)
        if n < 4:
            return remote(r1_s.at[sl, 2 * (1 - py) + n - 2, :, 128:256], rb_s.at[q, n - 2], ln_send.at[q, n], ln_recv.at[q, n], ynb)
        if n == 4:
            return remote(r1_s.at[sl, 2 * (1 - py) + px, :, 0:128], ra2_s.at[q], ln_send.at[q, n], ln_recv.at[q, n], ynb)
        return remote(r1_s.at[sl, 2 * py + 1 - px, :, 128:256], rb2_s.at[q], ln_send.at[q, n], ln_recv.at[q, n], xnb)

    def first_hop(i):
        for n in (0, 2, 1, 3):
            link(i, n).start()

    def second_hop(i):
        sl, q = i % SLOTS, i % LAG
        for n in range(2):
            link(i, n).wait_recv()
            r1_s[sl, 2 * n + px, :, 0:128] = r1_s[sl, 2 * n + px, :, 0:128] + ra_s[q, n]
        for n in range(2):
            link(i, n + 2).wait_recv()
            r1_s[sl, 2 * py + n, :, 128:256] = r1_s[sl, 2 * py + n, :, 128:256] + rb_s[q, n]
        link(i, 4).start()
        link(i, 5).start()

    def piece_out(i, first=False):
        dst = dwo.at[:, cols(i)] if first else dwq.at[:, cols(i - NJ)]
        return pltpu.make_async_copy(ost_s.at[i % 2], dst, osem.at[i % 2])

    def last_sum(i):
        sl, q = i % SLOTS, i % LAG

        @pl.when(i >= 2)
        def _():
            pltpu.make_async_copy(ost_s.at[i % 2], dwq.at[:, 0:C], osem.at[i % 2]).wait()

        link(i, 4).wait_recv()
        ost_s[i % 2, :, 0:128] = r1_s[sl, 2 * py + px, :, 0:128] + ra2_s[q]
        link(i, 5).wait_recv()
        ost_s[i % 2, :, 128:256] = r1_s[sl, 2 * py + px, :, 128:256] + rb2_s[q]
        for n in range(6):
            link(i, n).wait_send()

        @pl.when(i < NJ)
        def _():
            piece_out(i, True).start()

        @pl.when(i >= NJ)
        def _():
            piece_out(i).start()

    def pump(m, lo, hi):
        @pl.when((m - 4 >= lo) & (m - 4 < hi))
        def _():
            last_sum(m - 4)

        @pl.when((m - 2 >= lo) & (m - 2 < hi))
        def _():
            second_hop(m - 2)

        @pl.when((m >= lo) & (m < hi))
        def _():
            first_hop(m)

    gamma = gam[...].reshape(1, D)
    beta = bet[...].reshape(1, D)

    @pl.loop(0, NT_)
    def _(t):
        x_first(t).wait()
        for g in range(R // G):
            r = pl.ds(pl.multiple_of(t * R + G * g, G), G)
            x_hat, _ = normalise(qkv_s[0, r, :].astype(f32))
            u_s[r, :] = (x_hat * gamma + beta).astype(bf16)

    dy_all.start()

    def project(n, which, j, keep=False):
        w_in(n).wait()

        @pl.when(n + 2 < 3 * NJ)
        def _():
            w_in(n + 2).start()

        out = dot_nt(u_s[...], tile_s[slot(2 + n % 3), :]).astype(bf16)
        qkv_s[which, :, cols(j)] = out
        if keep:
            feat = phi(out.astype(f32)).astype(bf16)
            o_s[:, cols(j)] = feat
            zz_s[0, s, :, cols(j)] = jnp.sum(feat.astype(f32), axis=0, keepdims=True)

    def state(lo, hi):
        for j in range(lo, hi):
            p_s[BW * j:BW * j + BW, :] = dot_tn(o_s[:, BAND[j]:BAND[j] + BW], qkv_s[2, :, C * j:C * j + C])
            compact(p_s, BW * j, j)

    @pl.loop(0, 3)
    def _(n):
        project(n, 1, n, True)

    @pl.loop(3, 5)
    def _(n):
        project(n, 2, n - 3)

    state(0, 2)
    pl.semaphore_wait(barrier, 7)
    ar_start(0)

    @pl.loop(5, 7)
    def _(n):
        project(n, 1, n - 2, True)

    z_start(0)

    @pl.loop(7, 10)
    def _(n):
        project(n, 2, n - 5)

    ar_mid(0)
    state(2, 5)
    ar_start(1)

    @pl.loop(10, 13)
    def _(n):
        project(n, 0, n - 10)

    ar_mid(1)

    @pl.loop(13, 15)
    def _(n):
        project(n, 0, n - 10)

    wo_all.start()
    bd_s[...] = jnp.zeros((D, D), bf16)
    for j in range(NJ):
        hr = head_of(lax.broadcasted_iota(jnp.int32, (C, BW), 0) + C * j)
        hc = head_of(lax.broadcasted_iota(jnp.int32, (C, BW), 1) + BAND[j])
        on_s[j] = jnp.where(hr == hc, 1.0, 0.0).astype(bf16)

    z_end(0)
    ar_end(0)
    ar_end(1)
    expand()
    for j in range(NJ):
        z = c_s[HD:HD + 1, BAND[j]:BAND[j] + BW]
        zb_s[j] = jnp.where(on_s[j].astype(f32) > 0.5, jnp.broadcast_to(z, (C, BW)), 0.0).astype(bf16)

    def num_den(j):
        f = f_s[:, BAND[j]:BAND[j] + BW]
        return dot_nn(f, bd_s[BAND[j]:BAND[j] + BW, C * j:C * j + C]), dot_nt(f, zb_s[j])

    @pl.loop(0, NT_)
    def _(t):
        f_s[...] = phi(qkv_s[0, rows(t), :].astype(f32)).astype(bf16)
        for j in range(NJ):
            num, den = num_den(j)
            o_s[rows(t), C * j:C * j + C] = (num / den).astype(bf16)

    def y_tile(t):
        x_in(t).wait()

        @pl.when(t + 1 < NT_)
        def _():
            x_in(t + 1).start()

        @pl.when(t >= 2)
        def _():
            tile_out(y, t - 2).wait()

        sum_ = tile_s[slot(t % 2), :].astype(f32) + dot_nn(o_s[rows(t), :], wo_s[...])
        tile_s[slot(4 + t % 2), :] = sum_.astype(bf16)
        tile_out(y, t).start()

    x_in(0).start()
    dy_all.wait()
    wo_all.wait()

    @pl.loop(0, NJ)
    def _(i):
        product(i, o_s, g_s[:, cols(i)])

        @pl.when(i > 0)
        def _():
            chip_sum(i - 1)

        to_mate(i)

        @pl.when((i == 1) | (i == 3))
        def _():
            first_hop((i - 1) // 2)

    y_tile(0)
    chip_sum(NJ - 1)
    second_hop(0)
    first_hop(2)

    p_s[...] = jnp.zeros((2 * D, C), f32)
    gb_s[...] = jnp.zeros((2, 8, D), f32)

    @pl.loop(0, NT_)
    def _(t):
        acc_s[...] = dot_nt(g_s[rows(t), :], wo_s[...])
        f_s[...] = phi(qkv_s[0, rows(t), :].astype(f32)).astype(bf16)
        for j in range(NJ):
            cj = slice(C * j, C * j + C)
            den = dot_nt(f_s[:, BAND[j]:BAND[j] + BW], zb_s[j])
            den_s[:, cj] = den
            g_s[rows(t), cj] = (acc_s[:, cj] / den).astype(bf16)
        for j in range(NJ):
            cj = slice(C * j, C * j + C)
            band = slice(BAND[j], BAND[j] + BW)
            back = dot_nt(g_s[rows(t), band], bd_s[cj, band])
            acc_s[:, cj] = back
            prod = f_s[:, cj].astype(f32) / den_s[:, cj] * back
            high = prod.astype(bf16)
            ph_s[:, cj] = high
            pl_s[:, cj] = (prod - high.astype(f32)).astype(bf16)
        for j in range(NJ):
            cj = slice(C * j, C * j + C)
            band = slice(BAND[j], BAND[j] + BW)
            corr = dot_nt(ph_s[:, band], on_s[j]) + dot_nt(pl_s[:, band], on_s[j])
            d_f = acc_s[:, cj] - corr * c_s[HD:HD + 1, cj].astype(bf16).astype(f32)
            raw = qkv_s[0, rows(t), cj].astype(f32)
            qkv_s[0, rows(t), cj] = (d_f * slope(raw)).astype(bf16)
            gb_s[0, 0:1, cj] = gb_s[0, 0:1, cj] + jnp.sum(corr * f_s[:, cj].astype(f32), axis=0, keepdims=True)
            p_s[BW * j:BW * j + BW, :] = p_s[BW * j:BW * j + BW, :] + dot_tn(f_s[:, band], g_s[rows(t), cj])

        @pl.when(t % 2 == 1)
        def _():
            pump(3 + t // 2, 0, NJ)

    for j in range(NJ):
        compact(p_s, BW * j, j)
    zz_s[1, s] = -gb_s[0, 0:1, :]
    ar_start(2)
    z_start(1)
    wt_hi.start()

    def weight_chunk(i):
        n = i - NJ
        product(i, u_s, qkv_s[n // NJ, :, cols(n % NJ)])

    @pl.loop(NJ, 2 * NJ)
    def _(i):
        weight_chunk(i)

        @pl.when(i > NJ)
        def _():
            chip_sum(i - 1)

        to_mate(i)

        @pl.when((i == NJ + 1) | (i == NJ + 3))
        def _():
            first_hop(NJ + (i - NJ) // 2)

        @pl.when(i < NJ + 2)
        def _():
            last_sum(i - 2)

        @pl.when(i == NJ + 2)
        def _():
            ar_mid(2)


    @pl.loop(1, 3)
    def _(t):
        y_tile(t)

    z_end(1)
    ar_end(2)
    chip_sum(2 * NJ - 1)
    pump(NJ + 2, NJ, NCH)
    expand()

    @pl.loop(0, NT_)
    def _(t):
        f_s[...] = phi(qkv_s[1, rows(t), :].astype(f32)).astype(bf16)
        ph_s[...] = qkv_s[2, rows(t), :]
        for j in range(NJ):
            cj = slice(C * j, C * j + C)
            band = slice(BAND[j], BAND[j] + BW)
            d_f = dot_nt(ph_s[:, band], bd_s[cj, band]) + c_s[HD:HD + 1, cj]
            raw = qkv_s[1, rows(t), cj].astype(f32)
            qkv_s[1, rows(t), cj] = (d_f * slope(raw)).astype(bf16)
            qkv_s[2, rows(t), cj] = dot_nn(f_s[:, band], bd_s[band, cj]).astype(bf16)

        @pl.when((t == 3) | (t == 7))
        def _():
            pump(NJ + 3 + t // 7, NJ, NCH)

    @pl.loop(3, NT_)
    def _(t):
        @pl.when(t % 2 == 1)
        def _():
            i = 2 * NJ + (t - 3) // 2
            weight_chunk(i)

            @pl.when(i > 2 * NJ)
            def _():
                chip_sum(i - 1)

            to_mate(i)

            @pl.when(i == 2 * NJ + 1)
            def _():
                pump(2 * NJ, NJ, NCH)

        y_tile(t)

    wt_lo.start()
    tile_out(y, NT_ - 2).wait()
    tile_out(y, NT_ - 1).wait()
    gb_s[...] = jnp.zeros((2, 8, D), f32)
    x_in(0).start()
    dy_in(0).start()

    @pl.loop(0, NT_)
    def _(t):
        @pl.when(t < 7)
        def _():
            weight_chunk(2 * NJ + 3 + t)

        @pl.when(t < 7)
        def _():
            chip_sum(2 * NJ + 2 + t)
            to_mate(2 * NJ + 3 + t)

        @pl.when(t < NT_ - 1)
        def _():
            pump(2 * NJ + 1 + t + (t + 6) // 8, NJ, NCH)
        @pl.when(t == 0)
        def _():
            wt_lo.wait()
            wt_hi.wait()

        x_in(t).wait()
        dy_in(t).wait()

        @pl.when(t + 1 < NT_)
        def _():
            x_in(t + 1).start()
            dy_in(t + 1).start()

        @pl.when(t >= 2)
        def _():
            tile_out(dx, t - 2).wait()

        cut = T - D

        @pl.loop(0, NJ)
        def _(j):
            cj = cols(j)
            acc_s[:, cj] = (dot_nn(qkv_s[0, rows(t), :], o_s[0:D, cj])
                            + dot_nn(qkv_s[1, rows(t), 0:cut], o_s[D:T, cj])
                            + dot_nn(qkv_s[1, rows(t), cut:D], g_s[0:D - cut, cj])
                            + dot_nn(qkv_s[2, rows(t), :], g_s[D - cut:2 * D - cut, cj]))

        @pl.when(t == 6)
        def _():
            chip_sum(NCH - 1)

        @pl.when((t == 1) | (t >= 6))
        def _():
            pump(2 * NJ + 2 + t + t // 6, NJ, NCH)

        for g in range(R // G):
            gs = slice(G * g, G * g + G)
            x_hat, inv = normalise(tile_s[pl.ds(pl.multiple_of((t % 2) * R + G * g, G), G), :].astype(f32))
            du = acc_s[gs, :]
            dux = du * x_hat
            gb_s[0] = gb_s[0] + sum(dux[8 * q:8 * q + 8, :] for q in range(G // 8))
            gb_s[1] = gb_s[1] + sum(du[8 * q:8 * q + 8, :] for q in range(G // 8))
            e = du * gamma
            m1 = jnp.mean(e, axis=-1, keepdims=True)
            m2 = jnp.mean(e * x_hat, axis=-1, keepdims=True)
            tile_s[pl.ds(pl.multiple_of((4 + t % 2) * R + G * g, G), G), :] = (tile_s[pl.ds(pl.multiple_of((2 + t % 2) * R + G * g, G), G), :].astype(f32) + inv * (e - m1 - x_hat * m2)).astype(bf16)

        tile_out(dx, t).start()

    def gb_copy(k):
        return remote(gbr_s.at[0], gbr_s.at[k], gb_send.at[k], gb_recv.at[k], (s + k) % 8)

    for n in range(2):
        gbr_s[0, n:n + 1, :] = jnp.sum(gb_s[n], axis=0, keepdims=True)
    for k in range(1, 8):
        gb_copy(k).start()

    @pl.loop(NCH + 1, NCH + 4)
    def _(m):
        pump(m, NJ, NCH)

    tile_out(dx, NT_ - 2).wait()
    tile_out(dx, NT_ - 1).wait()
    for k in range(1, 8):
        gb_copy(k).wait_recv()
        gb_copy(k).wait_send()
    total = jnp.zeros((2, D), f32)
    for d in range(8):
        total = total + gbr_s[(s + 8 - d) % 8]
    dgam[...] = total[0]
    dbet[...] = total[1]
    piece_out(NCH - 2).wait()
    piece_out(NCH - 1).wait()


def local_block(x_tok, dy_tok, ln_gamma, ln_beta, w_qkv, w_out):
    w_t = jnp.transpose(w_qkv, (1, 2, 3, 0)).reshape(3 * D, D)
    hbm = pl.BlockSpec(memory_space=pl.ANY)
    vmem = pl.BlockSpec(memory_space=pltpu.VMEM)
    dma = pltpu.SemaphoreType.DMA
    scratch = [
        pltpu.VMEM((T, D), bf16),
        pltpu.VMEM((T, D), bf16),
        pltpu.VMEM((T, D), bf16),
        pltpu.VMEM((3, T, D), bf16),
        pltpu.VMEM((D, D), bf16),
        pltpu.VMEM((D, D), bf16),
        pltpu.VMEM((NJ, C, BW), bf16),
        pltpu.VMEM((NJ, C, BW), bf16),
        pltpu.VMEM((6 * R, D), bf16),
        pltpu.VMEM((R, D), bf16),
        pltpu.VMEM((R, D), f32),
        pltpu.VMEM((R, D), f32),
        pltpu.VMEM((R, D), bf16),
        pltpu.VMEM((R, D), bf16),
        pltpu.VMEM((HD + 8, D), f32),
        pltpu.VMEM((2, 8, 1, D), f32),
        pltpu.VMEM((8, 13, 8, 128), f32),
        pltpu.VMEM((8, 13, 8, 128), f32),
        pltpu.VMEM((8, 13, 8, 128), bf16),
        pltpu.VMEM((8, 2, D), f32),
        pltpu.VMEM((2, 8, D), f32),
        pltpu.VMEM((2 * D, C), f32),
        pltpu.VMEM((SLOTS, 4, PIECE, C), f32),
        pltpu.VMEM((LAG, 2, PIECE, 128), f32),
        pltpu.VMEM((LAG, 2, PIECE, 128), f32),
        pltpu.VMEM((LAG, PIECE, 128), f32),
        pltpu.VMEM((LAG, PIECE, 128), f32),
        pltpu.VMEM((2, PIECE, C), f32),
        dma((NT_,)), dma((2,)), dma((2,)), dma((2,)), dma((3,)), dma((3,)), dma((2,)),
        dma((2, 8)), dma((2, 8)), dma((3, 2, 8)), dma((3, 2, 8)), dma((8,)), dma((8,)),
        dma((2, 4)), dma((2, 4)), dma((LAG, 6)), dma((LAG, 6)),
    ]
    y, dx, dwq, dwo, dgam, dbet = pl.pallas_call(
        block,
        name="block",
        out_shape=(jax.ShapeDtypeStruct((T, D), bf16), jax.ShapeDtypeStruct((T, D), bf16),
                   jax.ShapeDtypeStruct((PIECE, 3 * D), f32), jax.ShapeDtypeStruct((PIECE, D), f32),
                   jax.ShapeDtypeStruct((D,), f32), jax.ShapeDtypeStruct((D,), f32)),
        in_specs=[hbm, hbm, hbm, hbm, vmem, vmem],
        out_specs=(hbm, hbm, hbm, hbm, vmem, vmem),
        scratch_shapes=scratch,
        compiler_params=pltpu.CompilerParams(collective_id=0, has_side_effects=True, vmem_limit_bytes=67043328),
    )(x_tok, dy_tok, w_t, w_out, ln_gamma, ln_beta)
    return (y, dx, dwq.reshape(PIECE, 3, NH, HD), dwo, dgam, dbet)


def solution(mesh):
    rows = P(("data", "seq"), None)
    return jax.shard_map(
        local_block, mesh=mesh,
        in_specs=(rows, rows, P(None), P(None), P(None, None, None, None), P(None, None)),
        out_specs=(rows, rows, P(("data", "seq"), None, None, None), rows, P("data"), P("data")),
        check_vma=False)
```

```python
import functools

import jax
import jax.numpy as jnp
from jax import lax
from jax.experimental import pallas as pl
from jax.experimental.pallas import tpu as pltpu
from jax.sharding import PartitionSpec as P

LN_EPS = 1e-5
T = 2048
D = 1280
HD = 80
NH = 16
R = 256
G = 32
NT_ = T // R
C = 256
NJ = D // C
BW = 512
BAND = [min(max(C * j - 128, 0), D - BW) for j in range(NJ)]
PIECE = D // 8
NCH = 4 * NJ
SLOTS = 8
LAG = 4
f32 = jnp.float32
bf16 = jnp.bfloat16


def dot_nn(a, b):
    return lax.dot_general(a, b, (((1,), (0,)), ((), ())), preferred_element_type=f32)


def dot_nt(a, b):
    return lax.dot_general(a, b, (((1,), (1,)), ((), ())), preferred_element_type=f32)


def dot_tn(a, b):
    return lax.dot_general(a, b, (((0,), (0,)), ((), ())), preferred_element_type=f32)


def phi(t):
    return jnp.where(t > 0, t + 1.0, jnp.exp(jnp.minimum(t, 0.0)))


def slope(t):
    return jnp.where(t > 0, 1.0, jnp.exp(jnp.minimum(t, 0.0)))


def head_of(idx):
    return (idx * 6554) >> 19


def normalise(x):
    centered = x - jnp.mean(x, axis=-1, keepdims=True)
    inv = lax.rsqrt(jnp.mean(centered * centered, axis=-1, keepdims=True) + LN_EPS)
    return centered * inv, inv


def block(x, dy, w_t, w_o, gam, bet,
          y, dx, dwq, dwo, dgam, dbet,
          u_s, g_s, o_s, qkv_s, wo_s, bd_s, zb_s, on_s, tile_s,
          f_s, acc_s, den_s, ph_s, pl_s, c_s, zz_s, part_s, rsr_s, ag_s, gbr_s, gb_s,
          p_s, r1_s, ra_s, rb_s, ra2_s, rb2_s, ost_s,
          fsem, xsem, dsem, ysem, wsem, lsem, osem, z_send, z_recv, ar_send, ar_recv, gb_send, gb_recv,
          dd_send, dd_recv, ln_send, ln_recv):
    s = lax.axis_index("seq")
    core = s % 2
    px = (s // 2) % 2
    py = s // 4
    mate = s + 1 - 2 * core
    xnb = s + 2 - 4 * px
    ynb = s + 4 - 8 * py

    def remote(src, dst, ssem, rsem, dev):
        return pltpu.make_async_remote_copy(src_ref=src, dst_ref=dst, send_sem=ssem, recv_sem=rsem,
                                            device_id={"seq": dev}, device_id_type=pl.DeviceIdType.MESH)

    def rows(t):
        return pl.ds(pl.multiple_of(t * R, R), R)

    def cols(j):
        return pl.ds(pl.multiple_of(j * C, C), C)

    def slot(n):
        return pl.ds(pl.multiple_of(n * R, R), R)

    def x_in(t):
        return pltpu.make_async_copy(x.at[rows(t), :], tile_s.at[slot(t % 2), :], xsem.at[t % 2])

    def dy_in(t):
        return pltpu.make_async_copy(dy.at[rows(t), :], tile_s.at[slot(2 + t % 2), :], dsem.at[t % 2])

    def tile_out(dst, t):
        return pltpu.make_async_copy(tile_s.at[slot(4 + t % 2), :], dst.at[rows(t), :], ysem.at[t % 2])

    def w_in(n):
        def ge(k):
            return int(n >= k) if isinstance(n, int) else (n >= k).astype(jnp.int32)

        r = n + 5 + 2 * ge(3) - 4 * ge(5) + 2 * ge(7) - 15 * ge(10)
        return pltpu.make_async_copy(w_t.at[cols(r), :], tile_s.at[slot(2 + n % 3), :], wsem.at[n % 3])

    dy_all = pltpu.make_async_copy(dy, g_s, lsem.at[0])
    wo_all = pltpu.make_async_copy(w_o, wo_s, lsem.at[1])
    wt_lo = pltpu.make_async_copy(w_t.at[pl.ds(0, T), :], o_s, lsem.at[2])
    wt_hi = pltpu.make_async_copy(w_t.at[pl.ds(T, 3 * D - T), :], g_s.at[pl.ds(0, 3 * D - T), :], lsem.at[0])

    def x_first(t):
        return pltpu.make_async_copy(x.at[rows(t), :], qkv_s.at[0, rows(t), :], fsem.at[t])

    for t in range(NT_):
        x_first(t).start()
        if t == 1:
            w_in(0).start()
            w_in(1).start()

    barrier = pltpu.get_barrier_semaphore()
    for k in range(1, 8):
        pl.semaphore_signal(barrier, inc=1, device_id={"seq": (s + k) % 8}, device_id_type=pl.DeviceIdType.MESH)

    tiles = [[(r, c) for r in range(10) for c in cs] for cs in (range(4), range(4, 10), range(10))]
    share = ((0, 5), (5, 13), (0, 13))

    def place(a, m):
        lo, hi = share[a]
        return m // (hi - lo), lo + m % (hi - lo)

    def ar_copy(a, phase, k, landing=False):
        dev = (s + 8 - k) % 8 if landing else (s + k) % 8
        lo, hi = share[a]
        sems = ar_send.at[a, phase, k], ar_recv.at[a, phase, k], dev
        if phase == 0:
            row = dev if landing else s
            return remote(part_s.at[dev, lo:hi], rsr_s.at[row, lo:hi], *sems)
        row = dev if landing else s
        return remote(ag_s.at[row, lo:hi], ag_s.at[row, lo:hi], *sems)

    def z_copy(b, k, landing=False):
        dev = (s + 8 - k) % 8 if landing else (s + k) % 8
        row = dev if landing else s
        return remote(zz_s.at[b, row], zz_s.at[b, row], z_send.at[b, k], z_recv.at[b, k], dev)

    def z_start(b):
        for k in range(1, 8):
            z_copy(b, k).start()

    def z_end(b):
        for k in range(1, 8):
            z_copy(b, k, True).wait_recv()
        for k in range(1, 8):
            z_copy(b, k).wait_send()
        total = zz_s[b, 0]
        for d in range(1, 8):
            total = total + zz_s[b, d]
        c_s[HD:HD + 1, :] = total

    def ar_start(a):
        for m, (r, c) in enumerate(tiles[a]):
            d, p = place(a, m)
            part_s[d, p] = c_s[8 * r:8 * r + 8, 128 * c:128 * c + 128]
        for k in range(1, 8):
            ar_copy(a, 0, k).start()

    def ar_mid(a):
        lo, hi = share[a]
        total = part_s[s, lo:hi]
        for k in range(1, 8):
            ar_copy(a, 0, k, True).wait_recv()
            total = total + rsr_s[(s + 8 - k) % 8, lo:hi]
        ag_s[s, lo:hi] = total.astype(bf16)
        for k in range(1, 8):
            ar_copy(a, 1, k).start()

    def ar_end(a):
        for k in range(1, 8):
            ar_copy(a, 1, k, True).wait_recv()
        for k in range(1, 8):
            ar_copy(a, 0, k).wait_send()
            ar_copy(a, 1, k).wait_send()
        for m, (r, c) in enumerate(tiles[a]):
            d, p = place(a, m)
            c_s[8 * r:8 * r + 8, 128 * c:128 * c + 128] = ag_s[d, p].astype(f32)

    def compact(ref, base, j):
        head = head_of(lax.broadcasted_iota(jnp.int32, (HD, C), 1) + C * j)
        out = jnp.zeros((HD, C), f32)
        for h in range(C * j // HD, (C * j + C - 1) // HD + 1):
            r0 = base + HD * h - BAND[j]
            out = jnp.where(head == h, ref[r0:r0 + HD, :], out)
        c_s[0:HD, C * j:C * j + C] = out

    def expand():
        for h in range(NH):
            c0 = HD * h // 128 * 128
            c1 = -(-(HD * h + HD) // 128) * 128
            head = head_of(lax.broadcasted_iota(jnp.int32, (HD, c1 - c0), 1) + c0)
            bd_s[HD * h:HD * h + HD, c0:c1] = jnp.where(head == h, c_s[0:HD, c0:c1], 0.0).astype(bf16)

    def product(i, lhs, rhs):
        p_s[pl.ds(pl.multiple_of((i % 2) * D, D), D), :] = dot_tn(lhs[...], rhs)

    def dd(i, k):
        src = p_s.at[pl.ds(pl.multiple_of((i % 2) * D + (2 * k + 1 - core) * PIECE, 8), PIECE), :]
        return remote(src, r1_s.at[i % SLOTS, k], dd_send.at[i % 2, k], dd_recv.at[i % 2, k], mate)

    def to_mate(i):
        for k in range(4):
            dd(i, k).start()

    def chip_sum(i):
        for k in range(4):
            dd(i, k).wait_recv()
            own = pl.ds(pl.multiple_of((i % 2) * D + (2 * k + core) * PIECE, 8), PIECE)
            r1_s[i % SLOTS, k] = r1_s[i % SLOTS, k] + p_s[own, :]
            dd(i, k).wait_send()

    def link(i, n):
        sl, q = i % SLOTS, i % LAG
        if n < 2:
            return remote(r1_s.at[sl, 2 * n + 1 - px, :, 0:128], ra_s.at[q, n], ln_send.at[q, n], ln_recv.at[q, n], xnb)
        if n < 4:
            return remote(r1_s.at[sl, 2 * (1 - py) + n - 2, :, 128:256], rb_s.at[q, n - 2], ln_send.at[q, n], ln_recv.at[q, n], ynb)
        if n == 4:
            return remote(r1_s.at[sl, 2 * (1 - py) + px, :, 0:128], ra2_s.at[q], ln_send.at[q, n], ln_recv.at[q, n], ynb)
        return remote(r1_s.at[sl, 2 * py + 1 - px, :, 128:256], rb2_s.at[q], ln_send.at[q, n], ln_recv.at[q, n], xnb)

    def first_hop(i):
        for n in (0, 2, 1, 3):
            link(i, n).start()

    def second_hop(i):
        sl, q = i % SLOTS, i % LAG
        for n in range(2):
            link(i, n).wait_recv()
            r1_s[sl, 2 * n + px, :, 0:128] = r1_s[sl, 2 * n + px, :, 0:128] + ra_s[q, n]
        for n in range(2):
            link(i, n + 2).wait_recv()
            r1_s[sl, 2 * py + n, :, 128:256] = r1_s[sl, 2 * py + n, :, 128:256] + rb_s[q, n]
        link(i, 4).start()
        link(i, 5).start()

    def piece_out(i, first=False):
        dst = dwo.at[:, cols(i)] if first else dwq.at[:, cols(i - NJ)]
        return pltpu.make_async_copy(ost_s.at[i % 2], dst, osem.at[i % 2])

    def last_sum(i):
        sl, q = i % SLOTS, i % LAG

        @pl.when(i >= 2)
        def _():
            pltpu.make_async_copy(ost_s.at[i % 2], dwq.at[:, 0:C], osem.at[i % 2]).wait()

        link(i, 4).wait_recv()
        ost_s[i % 2, :, 0:128] = r1_s[sl, 2 * py + px, :, 0:128] + ra2_s[q]
        link(i, 5).wait_recv()
        ost_s[i % 2, :, 128:256] = r1_s[sl, 2 * py + px, :, 128:256] + rb2_s[q]
        for n in range(6):
            link(i, n).wait_send()

        @pl.when(i < NJ)
        def _():
            piece_out(i, True).start()

        @pl.when(i >= NJ)
        def _():
            piece_out(i).start()

    def pump(m, lo, hi):
        @pl.when((m - 4 >= lo) & (m - 4 < hi))
        def _():
            last_sum(m - 4)

        @pl.when((m - 2 >= lo) & (m - 2 < hi))
        def _():
            second_hop(m - 2)

        @pl.when((m >= lo) & (m < hi))
        def _():
            first_hop(m)

    gamma = gam[...].reshape(1, D)
    beta = bet[...].reshape(1, D)

    @pl.loop(0, NT_)
    def _(t):
        x_first(t).wait()
        for g in range(R // G):
            r = pl.ds(pl.multiple_of(t * R + G * g, G), G)
            x_hat, _ = normalise(qkv_s[0, r, :].astype(f32))
            u_s[r, :] = (x_hat * gamma + beta).astype(bf16)

    dy_all.start()

    def project(n, which, j, keep=False):
        w_in(n).wait()

        @pl.when(n + 2 < 3 * NJ)
        def _():
            w_in(n + 2).start()

        out = dot_nt(u_s[...], tile_s[slot(2 + n % 3), :]).astype(bf16)
        qkv_s[which, :, cols(j)] = out
        if keep:
            feat = phi(out.astype(f32)).astype(bf16)
            o_s[:, cols(j)] = feat
            zz_s[0, s, :, cols(j)] = jnp.sum(feat.astype(f32), axis=0, keepdims=True)

    def state(lo, hi):
        for j in range(lo, hi):
            p_s[BW * j:BW * j + BW, :] = dot_tn(o_s[:, BAND[j]:BAND[j] + BW], qkv_s[2, :, C * j:C * j + C])
            compact(p_s, BW * j, j)

    @pl.loop(0, 3)
    def _(n):
        project(n, 1, n, True)

    @pl.loop(3, 5)
    def _(n):
        project(n, 2, n - 3)

    state(0, 2)
    pl.semaphore_wait(barrier, 7)
    ar_start(0)

    @pl.loop(5, 7)
    def _(n):
        project(n, 1, n - 2, True)

    z_start(0)

    @pl.loop(7, 10)
    def _(n):
        project(n, 2, n - 5)

    ar_mid(0)
    state(2, 5)
    ar_start(1)

    @pl.loop(10, 13)
    def _(n):
        project(n, 0, n - 10)

    ar_mid(1)

    @pl.loop(13, 15)
    def _(n):
        project(n, 0, n - 10)

    wo_all.start()
    bd_s[...] = jnp.zeros((D, D), bf16)
    for j in range(NJ):
        hr = head_of(lax.broadcasted_iota(jnp.int32, (C, BW), 0) + C * j)
        hc = head_of(lax.broadcasted_iota(jnp.int32, (C, BW), 1) + BAND[j])
        on_s[j] = jnp.where(hr == hc, 1.0, 0.0).astype(bf16)

    z_end(0)
    ar_end(0)
    ar_end(1)
    expand()
    for j in range(NJ):
        z = c_s[HD:HD + 1, BAND[j]:BAND[j] + BW]
        zb_s[j] = jnp.where(on_s[j].astype(f32) > 0.5, jnp.broadcast_to(z, (C, BW)), 0.0).astype(bf16)

    def num_den(j):
        f = f_s[:, BAND[j]:BAND[j] + BW]
        return dot_nn(f, bd_s[BAND[j]:BAND[j] + BW, C * j:C * j + C]), dot_nt(f, zb_s[j])

    @pl.loop(0, NT_)
    def _(t):
        f_s[...] = phi(qkv_s[0, rows(t), :].astype(f32)).astype(bf16)
        for j in range(NJ):
            num, den = num_den(j)
            o_s[rows(t), C * j:C * j + C] = (num / den).astype(bf16)

    def y_tile(t):
        x_in(t).wait()

        @pl.when(t + 1 < NT_)
        def _():
            x_in(t + 1).start()

        @pl.when(t >= 2)
        def _():
            tile_out(y, t - 2).wait()

        sum_ = tile_s[slot(t % 2), :].astype(f32) + dot_nn(o_s[rows(t), :], wo_s[...])
        tile_s[slot(4 + t % 2), :] = sum_.astype(bf16)
        tile_out(y, t).start()

    x_in(0).start()
    dy_all.wait()
    wo_all.wait()

    @pl.loop(0, NJ)
    def _(i):
        product(i, o_s, g_s[:, cols(i)])

        @pl.when(i > 0)
        def _():
            chip_sum(i - 1)

        to_mate(i)

        @pl.when((i == 1) | (i == 3))
        def _():
            first_hop((i - 1) // 2)

    y_tile(0)
    chip_sum(NJ - 1)
    second_hop(0)
    first_hop(2)

    p_s[...] = jnp.zeros((2 * D, C), f32)
    gb_s[...] = jnp.zeros((2, 8, D), f32)

    @pl.loop(0, NT_)
    def _(t):
        acc_s[...] = dot_nt(g_s[rows(t), :], wo_s[...])
        f_s[...] = phi(qkv_s[0, rows(t), :].astype(f32)).astype(bf16)
        for j in range(NJ):
            cj = slice(C * j, C * j + C)
            den = dot_nt(f_s[:, BAND[j]:BAND[j] + BW], zb_s[j])
            den_s[:, cj] = den
            g_s[rows(t), cj] = (acc_s[:, cj] / den).astype(bf16)
        for j in range(NJ):
            cj = slice(C * j, C * j + C)
            band = slice(BAND[j], BAND[j] + BW)
            back = dot_nt(g_s[rows(t), band], bd_s[cj, band])
            acc_s[:, cj] = back
            prod = f_s[:, cj].astype(f32) / den_s[:, cj] * back
            high = prod.astype(bf16)
            ph_s[:, cj] = high
            pl_s[:, cj] = (prod - high.astype(f32)).astype(bf16)
        for j in range(NJ):
            cj = slice(C * j, C * j + C)
            band = slice(BAND[j], BAND[j] + BW)
            corr = dot_nt(ph_s[:, band], on_s[j]) + dot_nt(pl_s[:, band], on_s[j])
            d_f = acc_s[:, cj] - corr * c_s[HD:HD + 1, cj].astype(bf16).astype(f32)
            raw = qkv_s[0, rows(t), cj].astype(f32)
            qkv_s[0, rows(t), cj] = (d_f * slope(raw)).astype(bf16)
            gb_s[0, 0:1, cj] = gb_s[0, 0:1, cj] + jnp.sum(corr * f_s[:, cj].astype(f32), axis=0, keepdims=True)
            p_s[BW * j:BW * j + BW, :] = p_s[BW * j:BW * j + BW, :] + dot_tn(f_s[:, band], g_s[rows(t), cj])

        @pl.when(t % 2 == 1)
        def _():
            pump(3 + t // 2, 0, NJ)

    for j in range(NJ):
        compact(p_s, BW * j, j)
    zz_s[1, s] = -gb_s[0, 0:1, :]
    ar_start(2)
    z_start(1)
    wt_hi.start()

    def weight_chunk(i):
        n = i - NJ
        product(i, u_s, qkv_s[n // NJ, :, cols(n % NJ)])

    @pl.loop(NJ, 2 * NJ)
    def _(i):
        weight_chunk(i)

        @pl.when(i > NJ)
        def _():
            chip_sum(i - 1)

        to_mate(i)

        @pl.when((i == NJ + 1) | (i == NJ + 3))
        def _():
            first_hop(NJ + (i - NJ) // 2)

        @pl.when(i < NJ + 2)
        def _():
            last_sum(i - 2)

        @pl.when(i == NJ + 2)
        def _():
            ar_mid(2)


    @pl.loop(1, 3)
    def _(t):
        y_tile(t)

    z_end(1)
    ar_end(2)
    chip_sum(2 * NJ - 1)
    pump(NJ + 2, NJ, NCH)
    expand()

    @pl.loop(0, NT_)
    def _(t):
        f_s[...] = phi(qkv_s[1, rows(t), :].astype(f32)).astype(bf16)
        ph_s[...] = qkv_s[2, rows(t), :]
        for j in range(NJ):
            cj = slice(C * j, C * j + C)
            band = slice(BAND[j], BAND[j] + BW)
            d_f = dot_nt(ph_s[:, band], bd_s[cj, band]) + c_s[HD:HD + 1, cj]
            raw = qkv_s[1, rows(t), cj].astype(f32)
            qkv_s[1, rows(t), cj] = (d_f * slope(raw)).astype(bf16)
            qkv_s[2, rows(t), cj] = dot_nn(f_s[:, band], bd_s[band, cj]).astype(bf16)

        @pl.when((t == 3) | (t == 7))
        def _():
            pump(NJ + 3 + t // 7, NJ, NCH)

    @pl.loop(3, NT_)
    def _(t):
        @pl.when(t % 2 == 1)
        def _():
            i = 2 * NJ + (t - 3) // 2
            weight_chunk(i)

            @pl.when(i > 2 * NJ)
            def _():
                chip_sum(i - 1)

            to_mate(i)

            @pl.when(i > 2 * NJ)
            def _():
                pump(i - 1, NJ, NCH)

        y_tile(t)

    wt_lo.start()
    tile_out(y, NT_ - 2).wait()
    tile_out(y, NT_ - 1).wait()
    gb_s[...] = jnp.zeros((2, 8, D), f32)
    x_in(0).start()
    dy_in(0).start()

    @pl.loop(0, NT_)
    def _(t):
        @pl.when(t < 7)
        def _():
            weight_chunk(2 * NJ + 3 + t)

        @pl.when(t < 7)
        def _():
            chip_sum(2 * NJ + 2 + t)
            to_mate(2 * NJ + 3 + t)

        @pl.when(t < NT_ - 1)
        def _():
            pump(2 * NJ + 2 + t, NJ, NCH)
        @pl.when(t == 0)
        def _():
            wt_lo.wait()
            wt_hi.wait()

        x_in(t).wait()
        dy_in(t).wait()

        @pl.when(t + 1 < NT_)
        def _():
            x_in(t + 1).start()
            dy_in(t + 1).start()

        @pl.when(t >= 2)
        def _():
            tile_out(dx, t - 2).wait()

        cut = T - D

        @pl.loop(0, NJ)
        def _(j):
            cj = cols(j)
            acc_s[:, cj] = (dot_nn(qkv_s[0, rows(t), :], o_s[0:D, cj])
                            + dot_nn(qkv_s[1, rows(t), 0:cut], o_s[D:T, cj])
                            + dot_nn(qkv_s[1, rows(t), cut:D], g_s[0:D - cut, cj])
                            + dot_nn(qkv_s[2, rows(t), :], g_s[D - cut:2 * D - cut, cj]))

        @pl.when(t == 6)
        def _():
            chip_sum(NCH - 1)

        @pl.when(t >= 6)
        def _():
            pump(2 * NJ + 2 + t + t // 6, NJ, NCH)

        for g in range(R // G):
            gs = slice(G * g, G * g + G)
            x_hat, inv = normalise(tile_s[pl.ds(pl.multiple_of((t % 2) * R + G * g, G), G), :].astype(f32))
            du = acc_s[gs, :]
            dux = du * x_hat
            gb_s[0] = gb_s[0] + sum(dux[8 * q:8 * q + 8, :] for q in range(G // 8))
            gb_s[1] = gb_s[1] + sum(du[8 * q:8 * q + 8, :] for q in range(G // 8))
            e = du * gamma
            m1 = jnp.mean(e, axis=-1, keepdims=True)
            m2 = jnp.mean(e * x_hat, axis=-1, keepdims=True)
            tile_s[pl.ds(pl.multiple_of((4 + t % 2) * R + G * g, G), G), :] = (tile_s[pl.ds(pl.multiple_of((2 + t % 2) * R + G * g, G), G), :].astype(f32) + inv * (e - m1 - x_hat * m2)).astype(bf16)

        tile_out(dx, t).start()

    def gb_copy(k):
        return remote(gbr_s.at[0], gbr_s.at[k], gb_send.at[k], gb_recv.at[k], (s + k) % 8)

    for n in range(2):
        gbr_s[0, n:n + 1, :] = jnp.sum(gb_s[n], axis=0, keepdims=True)
    for k in range(1, 8):
        gb_copy(k).start()

    @pl.loop(NCH + 1, NCH + 4)
    def _(m):
        pump(m, NJ, NCH)

    tile_out(dx, NT_ - 2).wait()
    tile_out(dx, NT_ - 1).wait()
    for k in range(1, 8):
        gb_copy(k).wait_recv()
        gb_copy(k).wait_send()
    total = jnp.zeros((2, D), f32)
    for d in range(8):
        total = total + gbr_s[(s + 8 - d) % 8]
    dgam[...] = total[0]
    dbet[...] = total[1]
    piece_out(NCH - 2).wait()
    piece_out(NCH - 1).wait()


def local_block(x_tok, dy_tok, ln_gamma, ln_beta, w_qkv, w_out):
    w_t = jnp.transpose(w_qkv, (1, 2, 3, 0)).reshape(3 * D, D)
    hbm = pl.BlockSpec(memory_space=pl.ANY)
    vmem = pl.BlockSpec(memory_space=pltpu.VMEM)
    dma = pltpu.SemaphoreType.DMA
    scratch = [
        pltpu.VMEM((T, D), bf16),
        pltpu.VMEM((T, D), bf16),
        pltpu.VMEM((T, D), bf16),
        pltpu.VMEM((3, T, D), bf16),
        pltpu.VMEM((D, D), bf16),
        pltpu.VMEM((D, D), bf16),
        pltpu.VMEM((NJ, C, BW), bf16),
        pltpu.VMEM((NJ, C, BW), bf16),
        pltpu.VMEM((6 * R, D), bf16),
        pltpu.VMEM((R, D), bf16),
        pltpu.VMEM((R, D), f32),
        pltpu.VMEM((R, D), f32),
        pltpu.VMEM((R, D), bf16),
        pltpu.VMEM((R, D), bf16),
        pltpu.VMEM((HD + 8, D), f32),
        pltpu.VMEM((2, 8, 1, D), f32),
        pltpu.VMEM((8, 13, 8, 128), f32),
        pltpu.VMEM((8, 13, 8, 128), f32),
        pltpu.VMEM((8, 13, 8, 128), bf16),
        pltpu.VMEM((8, 2, D), f32),
        pltpu.VMEM((2, 8, D), f32),
        pltpu.VMEM((2 * D, C), f32),
        pltpu.VMEM((SLOTS, 4, PIECE, C), f32),
        pltpu.VMEM((LAG, 2, PIECE, 128), f32),
        pltpu.VMEM((LAG, 2, PIECE, 128), f32),
        pltpu.VMEM((LAG, PIECE, 128), f32),
        pltpu.VMEM((LAG, PIECE, 128), f32),
        pltpu.VMEM((2, PIECE, C), f32),
        dma((NT_,)), dma((2,)), dma((2,)), dma((2,)), dma((3,)), dma((3,)), dma((2,)),
        dma((2, 8)), dma((2, 8)), dma((3, 2, 8)), dma((3, 2, 8)), dma((8,)), dma((8,)),
        dma((2, 4)), dma((2, 4)), dma((LAG, 6)), dma((LAG, 6)),
    ]
    y, dx, dwq, dwo, dgam, dbet = pl.pallas_call(
        block,
        name="block",
        out_shape=(jax.ShapeDtypeStruct((T, D), bf16), jax.ShapeDtypeStruct((T, D), bf16),
                   jax.ShapeDtypeStruct((PIECE, 3 * D), f32), jax.ShapeDtypeStruct((PIECE, D), f32),
                   jax.ShapeDtypeStruct((D,), f32), jax.ShapeDtypeStruct((D,), f32)),
        in_specs=[hbm, hbm, hbm, hbm, vmem, vmem],
        out_specs=(hbm, hbm, hbm, hbm, vmem, vmem),
        scratch_shapes=scratch,
        compiler_params=pltpu.CompilerParams(collective_id=0, has_side_effects=True, vmem_limit_bytes=67043328),
    )(x_tok, dy_tok, w_t, w_out, ln_gamma, ln_beta)
    return (y, dx, dwq.reshape(PIECE, 3, NH, HD), dwo, dgam, dbet)


def solution(mesh):
    rows = P(("data", "seq"), None)
    return jax.shard_map(
        local_block, mesh=mesh,
        in_specs=(rows, rows, P(None), P(None), P(None, None, None, None), P(None, None)),
        out_specs=(rows, rows, P(("data", "seq"), None, None, None), rows, P("data"), P("data")),
        check_vma=False)
```
